32 devices in a mesh: grp: 2 (over y), seq: 4 (over z), head: 4 (over x, core).
Axes of the slice: x: 2, y: 2, z: 4, core: 2. Of those that a mesh axis runs over, the one named last changes fastest.
Arguments:
- queries: bfloat16 [1024, 32, 128], P(('grp', 'seq'), 'head'), parts along dimension 0, may hold values from -26 to 26
- keys: bfloat16 [1024, 8, 128], P(('grp', 'seq'), 'head'), parts along dimension 0, may hold values from -13 to 13
- values: bfloat16 [1024, 8, 128], P(('grp', 'seq'), 'head'), parts along dimension 0, may hold values from -6 to 6
- block_order: int32 [16], P('grp'), parts along dimension 0, may hold values from 0 to 7, as said below
Outputs:
- attended: bfloat16 [1024, 32, 128], P(('grp', 'seq'), 'head'), parts along dimension 0
The draws below stay inside these ranges and needn't reach their ends.
There are 2 independent parts, one for each index of `grp`. The reference program is written for one: setup_inputs(seed, part) draws one part's arguments, and reference() takes and returns one part's arrays. A program takes and returns all parts, laid end to end along the dimension named above; each array names one. Nothing has to cross between parts.
Inputs may be any that keep to these rules, and one draw needn't show every extreme that they name: `block_order`: slots 2 i and 2 i + 1 hold blocks c and 7 - c for some c, in either order; every block stands in one slot.
All inputs are finite; a program needn't handle non-finite values.
Results may differ from the reference program's by a relative error of at most 0.0055.
Values may be sent and summed in bfloat16 or wider, within the bound.
No kernel may reach another device: no remote copies, remote signals or barrier semaphores. Data moves between devices by JAX's collectives and lax.ppermute only.
A program may use at most 128 MiB of HBM per device.

```python
import jax
import jax.numpy as jnp
from jax import lax

QH = 32
KVH = 8
HD = 128
TOK_DEV = 128
BLOCK = 64
TOKENS = 512
N_SEQ = 4


def pair_order(key):
    count = N_SEQ
    shuffled = jax.random.permutation(jax.random.fold_in(key, 11), count).astype(jnp.int32)
    flips = jax.random.randint(jax.random.fold_in(key, 12), (count,), 0, 2).astype(jnp.int32)
    first = jnp.where(flips == 0, shuffled, 2 * count - 1 - shuffled)
    second = 2 * count - 1 - first
    return jnp.stack([first, second], axis=1).reshape(2 * count).astype(jnp.int32)


def draw_block_order(key, part):
    return pair_order(key)


def draw_queries(key, part):
    base = jnp.clip(jax.random.normal(jax.random.fold_in(key, 21), (TOKENS, QH, HD), jnp.float32), -5.0, 5.0)
    return base.astype(jnp.bfloat16)


def draw_keys(key, part):
    base = jnp.clip(jax.random.normal(jax.random.fold_in(key, 22), (TOKENS, KVH, HD), jnp.float32), -5.0, 5.0)
    return base.astype(jnp.bfloat16)


def levels(stream_key, shape, cuts, smallest, largest):
    gain = 1.0
    for position, parts in cuts:
        steps = jax.random.uniform(jax.random.fold_in(jax.random.fold_in(stream_key, 6), position), (parts,), jnp.float32, smallest / len(cuts), largest / len(cuts))
        gain = gain * jnp.repeat(jnp.exp(steps), shape[position] // parts).reshape((-1,) + (1,) * (len(shape) - 1 - position))
    return gain


def normal_values(own_key, shape, spread, most, pieces=(), kind=jnp.bfloat16):
    factor_of = levels(own_key, shape, pieces, -0.22, 0.18) if pieces else 1.0
    values = jax.random.normal(own_key, shape, jnp.float32) * spread * factor_of
    return jnp.minimum(jnp.maximum(values, -most), most).astype(kind)


def setup_inputs(seed: int = 0, part: int = 0) -> dict:
    arg_keys = jax.random.split(jax.random.key(seed), 5)
    part_splits = jax.random.split(jax.random.fold_in(arg_keys[4], part), 5)
    return {
        "queries": draw_queries(jax.random.fold_in(jax.random.fold_in(arg_keys[4], part), 71), part),
        "keys": draw_keys(jax.random.fold_in(jax.random.fold_in(arg_keys[4], part), 71), part),
        "values": normal_values(part_splits[2], (TOKENS, KVH, HD), 1.0, 6.0, ((0, 4), (1, 4))),
        "block_order": draw_block_order(jax.random.fold_in(jax.random.fold_in(arg_keys[4], part), 71), part),
    }


def reference(queries, keys, values, block_order):
    rows = jnp.arange(TOKENS, dtype=jnp.int32)
    positions = block_order[rows // BLOCK].astype(jnp.int32) * BLOCK + rows % BLOCK
    key_float = keys.astype(jnp.float32)
    value_float = values.astype(jnp.float32)
    group_size = QH // KVH
    score_scale = HD ** -0.5

    def one_block(index):
        start = (index * TOK_DEV).astype(jnp.int32)
        query_rows = lax.dynamic_slice_in_dim(queries, start, TOK_DEV, 0).astype(jnp.float32)
        query_rows = query_rows.reshape(TOK_DEV, KVH, group_size, HD)
        query_pos = lax.dynamic_slice_in_dim(positions, start, TOK_DEV, 0)
        scores = jnp.einsum("cghd,pgd->ghcp", query_rows, key_float) * score_scale
        visible = (positions[None, :] <= query_pos[:, None])[None, None]
        top = jnp.max(jnp.where(visible, scores, -1e30), axis=-1)
        weights = jnp.where(visible, jnp.exp(scores - top[..., None]), 0.0)
        total = jnp.sum(weights, axis=-1)
        rounded = lax.optimization_barrier(weights.astype(jnp.bfloat16)).astype(jnp.float32)
        summed = jnp.einsum("ghcp,pgd->ghcd", rounded, value_float)
        result = summed / total[..., None]
        return jnp.transpose(result, (2, 0, 1, 3)).reshape(TOK_DEV, QH, HD).astype(jnp.bfloat16)

    blocks = lax.map(one_block, jnp.arange(N_SEQ, dtype=jnp.int32))
    return blocks.reshape(TOKENS, QH, HD)
```

```python
import functools

import jax
import jax.numpy as jnp
from jax import lax
from jax.experimental import pallas as pl
from jax.experimental.pallas import tpu as pltpu
from jax.sharding import PartitionSpec as P

LOW = -1e30
LOG2E = 1.4426950408889634


def pick(table, index):
    value = jnp.int32(table[0])
    for place in range(1, len(table)):
        value = jnp.where(index == place, jnp.int32(table[place]), value)
    return value


def attend(query, key, value, lanes, scale, state, diagonal):
    groups, per_token = lanes
    rows = query.shape[0]
    keys = key.shape[0] // groups
    lane = lax.broadcasted_iota(jnp.int32, (keys, rows), 1)
    group = (lane % per_token) // (per_token // groups)
    both = lax.dot_general(
        key, query, (((1,), (1,)), ((), ())), preferred_element_type=jnp.float32
    )
    scores = both[:keys]
    for g in range(1, groups):
        scores = jnp.where(group == g, both[g * keys : (g + 1) * keys], scores)
    scores = scores * scale
    if diagonal:
        place = lax.broadcasted_iota(jnp.int32, (keys, rows), 0)
        scores = jnp.where(place <= lane // per_token, scores, LOW)
    top = jnp.max(scores, axis=0, keepdims=True)
    if state is not None:
        top = jnp.maximum(top, state[0])
    weights = jnp.exp2(scores - top)
    total = jnp.sum(weights, axis=0, keepdims=True)
    rounded = weights.astype(jnp.bfloat16)
    nothing = jnp.zeros_like(rounded)
    spread = jnp.concatenate(
        [jnp.where(group == g, rounded, nothing) for g in range(groups)], axis=0
    )
    product = lax.dot_general(
        value, spread, (((0,), (0,)), ((), ())), preferred_element_type=jnp.float32
    )
    if state is None:
        return top, total, product
    factor = jnp.exp2(state[0] - top)
    return top, state[1] * factor + total, state[2] * factor + product


def load(refs, slot):
    return tuple(ref[slot] for ref in refs)


def store(refs, slot, state):
    for ref, part in zip(refs, state, strict=True):
        ref[slot] = part


def rows_of(ref, slot):
    half = ref.shape[0] // 2
    return ref[pl.ds(pl.multiple_of(slot * half, half), half), :]


def own_kernel(lanes, scale, order, query, packed, top, total, acc):
    me = lax.axis_index("seq")
    refs = (top, total, acc)
    for slot in range(2):
        state = attend(
            rows_of(query, slot), packed[slot, 0], packed[slot, 1], lanes, scale, None, True
        )
        store(refs, slot, state)
    late = jnp.where(order[2 * me] < order[2 * me + 1], 1, 0)
    early = 1 - late
    state = attend(
        rows_of(query, late), packed[early, 0], packed[early, 1], lanes, scale, load(refs, late), False
    )
    store(refs, late, state)


def remote(lanes, scale, order, query, packed, refs, me, source):
    late = jnp.where(order[2 * me] < order[2 * me + 1], 1, 0)
    early = 1 - late
    source_late = jnp.where(order[2 * source] < order[2 * source + 1], 1, 0)
    source_early = 1 - source_late
    state = attend(
        rows_of(query, late),
        packed[source_early, 0],
        packed[source_early, 1],
        lanes,
        scale,
        load(refs, late),
        False,
    )
    store(refs, late, state)
    before = order[2 * source + source_early] < order[2 * me + early]
    mine = jnp.where(before, early, late)
    theirs = jnp.where(before, source_early, source_late)
    state = attend(
        rows_of(query, mine),
        packed[theirs, 0],
        packed[theirs, 1],
        lanes,
        scale,
        load(refs, mine),
        False,
    )
    store(refs, mine, state)


def finish(refs, out):
    half = out.shape[0] // 2
    for slot in range(2):
        result = refs[2][slot] / refs[1][slot]
        out[slot * half : (slot + 1) * half, :] = result.T.astype(out.dtype)


def middle_kernel(lanes, scale, sources, order, query, *rest):
    count = len(sources)
    blocks, before, after = rest[:count], rest[count : count + 3], rest[count + 3 :]
    me = lax.axis_index("seq")
    for slot in range(2):
        store(after, slot, load(before, slot))
    for table, packed in zip(sources, blocks, strict=True):
        remote(lanes, scale, order, query, packed, after, me, pick(table, me))


def last_kernel(lanes, scale, sources, choose, order, query, *rest):
    count = len(sources)
    blocks, before, out, after = rest[:count], rest[count : count + 3], rest[count + 3], rest[count + 4 :]
    me = lax.axis_index("seq")
    for slot in range(2):
        store(after, slot, load(before, slot))
    for number, (table, packed) in enumerate(zip(sources, blocks, strict=True)):
        @pl.when(pick(choose, me) == number)
        def _():
            remote(lanes, scale, order, query, packed, after, me, pick(table, me))
    finish(after, out)


def gathered_kernel(lanes, scale, order, query, blocks, *rest):
    before, out, after = rest[:3], rest[3], rest[4:]
    me = lax.axis_index("seq")
    count = blocks.shape[0]
    for slot in range(2):
        store(after, slot, load(before, slot))

    def step(index, carry):
        source = lax.rem(me + index, count)
        remote(lanes, scale, order, query, blocks.at[source], after, me, source)
        return carry

    lax.fori_loop(1, count, step, 0)
    finish(after, out)


def on_device(queries, keys, values, block_order):
    tokens, heads, width = queries.shape
    groups = keys.shape[1]
    half = tokens // 2
    devices = lax.axis_size("seq")
    scale = width ** (-0.5) * LOG2E
    lanes = (groups, heads)
    rows = tokens * heads
    query = queries.reshape(rows, width)

    def pack(array):
        split = array.reshape(2, half, groups, width)
        return jnp.transpose(split, (0, 2, 1, 3)).reshape(2, 1, groups * half, width)

    packed = jnp.concatenate([pack(keys), pack(values)], axis=1)
    shapes = [
        jax.ShapeDtypeStruct((2, 1, rows // 2), jnp.float32),
        jax.ShapeDtypeStruct((2, 1, rows // 2), jnp.float32),
        jax.ShapeDtypeStruct((2, width, rows // 2), jnp.float32),
    ]
    scratch = [pltpu.VMEM(s.shape, s.dtype) for s in shapes]
    result = jax.ShapeDtypeStruct((rows, width), queries.dtype)
    vmem = pl.BlockSpec(memory_space=pltpu.VMEM)
    smem = pl.BlockSpec(memory_space=pltpu.SMEM)

    def call(kernel, blocks, state, out_shape, tasks, scratch_shapes=()):
        inputs = [block_order, query, *blocks, *state]
        flops = 4 * tasks * groups * half * rows // 2 * width
        return pl.pallas_call(
            kernel,
            out_shape=out_shape,
            in_specs=[smem] + [vmem] * (len(inputs) - 1),
            out_specs=jax.tree.map(lambda _: vmem, out_shape),
            scratch_shapes=scratch_shapes,
            cost_estimate=pl.CostEstimate(
                flops=flops, bytes_accessed=rows * width * 2, transcendentals=tasks * half * rows
            ),
        )(*inputs)

    def permute(value, pairs):
        return lax.ppermute(value, "seq", pairs)

    if devices == 4:
        first = permute(packed, [(0, 2), (3, 1), (1, 0), (2, 3)])
        second = permute(packed, [(1, 3), (2, 0), (0, 1), (3, 2)])
        inner = permute(packed, [(1, 2), (2, 1), (0, 0), (3, 3)])
        state = call(functools.partial(own_kernel, lanes, scale), [packed], [], shapes, 3)
        outer = permute(first, [(2, 3), (1, 0), (0, 1), (3, 2)])
        state = call(
            functools.partial(middle_kernel, lanes, scale, [(1, 3, 0, 2), (2, 0, 3, 1)]),
            [first, second],
            state,
            shapes,
            4,
        )
        out = call(
            functools.partial(
                last_kernel, lanes, scale, [(0, 2, 1, 3), (3, 0, 3, 0)], (1, 0, 0, 1)
            ),
            [inner, outer],
            state,
            result,
            2,
            scratch,
        )
    else:
        blocks = lax.all_gather(packed, "seq", axis=0, tiled=False)
        state = call(functools.partial(own_kernel, lanes, scale), [packed], [], shapes, 3)
        out = call(
            functools.partial(gathered_kernel, lanes, scale), [blocks], state, result, 2 * devices, scratch
        )
    return out.reshape(tokens, heads, width)


def solution(mesh):
    placed = (
        P(("grp", "seq"), "head", None),
        P(("grp", "seq"), "head", None),
        P(("grp", "seq"), "head", None),
        P("grp"),
    )
    return jax.shard_map(
        on_device,
        mesh=mesh,
        in_specs=placed,
        out_specs=P(("grp", "seq"), "head", None),
        check_vma=False,
    )
```

```python
import functools

import jax
import jax.numpy as jnp
from jax import lax
from jax.experimental import pallas as pl
from jax.experimental.pallas import tpu as pltpu
from jax.sharding import PartitionSpec as P

LOW = -1e30
LOG2E = 1.4426950408889634


def pick(table, index):
    value = jnp.int32(table[0])
    for place in range(1, len(table)):
        value = jnp.where(index == place, jnp.int32(table[place]), value)
    return value


def attend(query, key, value, lanes, scale, state, diagonal):
    groups, per_token = lanes
    rows = query.shape[0]
    keys = key.shape[0] // groups
    lane = lax.broadcasted_iota(jnp.int32, (keys, rows), 1)
    group = (lane % per_token) // (per_token // groups)
    both = lax.dot_general(
        key, query, (((1,), (1,)), ((), ())), preferred_element_type=jnp.float32
    )
    scores = both[:keys]
    for g in range(1, groups):
        scores = jnp.where(group == g, both[g * keys : (g + 1) * keys], scores)
    scores = scores * scale
    if diagonal:
        place = lax.broadcasted_iota(jnp.int32, (keys, rows), 0)
        scores = jnp.where(place <= lane // per_token, scores, LOW)
    top = jnp.max(scores, axis=0, keepdims=True)
    if state is not None:
        top = jnp.maximum(top, state[0])
    weights = jnp.exp2(scores - top)
    total = jnp.sum(weights, axis=0, keepdims=True)
    rounded = weights.astype(jnp.bfloat16)
    nothing = jnp.zeros_like(rounded)
    spread = jnp.concatenate(
        [jnp.where(group == g, rounded, nothing) for g in range(groups)], axis=0
    )
    product = lax.dot_general(
        value, spread, (((0,), (0,)), ((), ())), preferred_element_type=jnp.float32
    )
    if state is None:
        return top, total, product
    factor = jnp.exp2(state[0] - top)
    return top, state[1] * factor + total, state[2] * factor + product


def load(refs, slot):
    return tuple(ref[slot] for ref in refs)


def store(refs, slot, state):
    for ref, part in zip(refs, state, strict=True):
        ref[slot] = part


def rows_of(ref, slot):
    half = ref.shape[0] // 2
    return ref[pl.ds(pl.multiple_of(slot * half, half), half), :]


def own_kernel(lanes, scale, order, query, packed, top, total, acc):
    me = lax.axis_index("seq")
    refs = (top, total, acc)
    for slot in range(2):
        state = attend(
            rows_of(query, slot), packed[slot, 0], packed[slot, 1], lanes, scale, None, True
        )
        store(refs, slot, state)
    late = jnp.where(order[2 * me] < order[2 * me + 1], 1, 0)
    early = 1 - late
    state = attend(
        rows_of(query, late), packed[early, 0], packed[early, 1], lanes, scale, load(refs, late), False
    )
    store(refs, late, state)


def remote(lanes, scale, order, query, packed, refs, me, source):
    late = jnp.where(order[2 * me] < order[2 * me + 1], 1, 0)
    early = 1 - late
    source_late = jnp.where(order[2 * source] < order[2 * source + 1], 1, 0)
    source_early = 1 - source_late
    state = attend(
        rows_of(query, late),
        packed[source_early, 0],
        packed[source_early, 1],
        lanes,
        scale,
        load(refs, late),
        False,
    )
    store(refs, late, state)
    before = order[2 * source + source_early] < order[2 * me + early]
    mine = jnp.where(before, early, late)
    theirs = jnp.where(before, source_early, source_late)
    state = attend(
        rows_of(query, mine),
        packed[theirs, 0],
        packed[theirs, 1],
        lanes,
        scale,
        load(refs, mine),
        False,
    )
    store(refs, mine, state)


def finish(refs, out):
    half = out.shape[0] // 2
    for slot in range(2):
        result = refs[2][slot] / refs[1][slot]
        out[slot * half : (slot + 1) * half, :] = result.T.astype(out.dtype)


def middle_kernel(lanes, scale, sources, order, query, *rest):
    count = len(sources)
    blocks, before, after = rest[:count], rest[count : count + 3], rest[count + 3 :]
    me = lax.axis_index("seq")
    for slot in range(2):
        store(after, slot, load(before, slot))
    for table, packed in zip(sources, blocks, strict=True):
        remote(lanes, scale, order, query, packed, after, me, pick(table, me))


def last_kernel(lanes, scale, sources, choose, order, query, *rest):
    count = len(sources)
    blocks, before, out, after = rest[:count], rest[count : count + 3], rest[count + 3], rest[count + 4 :]
    me = lax.axis_index("seq")
    for slot in range(2):
        store(after, slot, load(before, slot))
    for number, (table, packed) in enumerate(zip(sources, blocks, strict=True)):
        @pl.when(pick(choose, me) == number)
        def _():
            remote(lanes, scale, order, query, packed, after, me, pick(table, me))
    finish(after, out)


def gathered_kernel(lanes, scale, order, query, blocks, *rest):
    before, out, after = rest[:3], rest[3], rest[4:]
    me = lax.axis_index("seq")
    count = blocks.shape[0]
    for slot in range(2):
        store(after, slot, load(before, slot))

    def step(index, carry):
        source = lax.rem(me + index, count)
        remote(lanes, scale, order, query, blocks.at[source], after, me, source)
        return carry

    lax.fori_loop(1, count, step, 0)
    finish(after, out)


def on_device(queries, keys, values, block_order):
    tokens, heads, width = queries.shape
    groups = keys.shape[1]
    half = tokens // 2
    devices = lax.axis_size("seq")
    scale = width ** (-0.5) * LOG2E
    lanes = (groups, heads)
    rows = tokens * heads
    query = queries.reshape(rows, width)

    def pack(array):
        split = array.reshape(2, half, groups, width)
        return jnp.transpose(split, (0, 2, 1, 3)).reshape(2, 1, groups * half, width)

    packed = jnp.concatenate([pack(keys), pack(values)], axis=1)
    shapes = [
        jax.ShapeDtypeStruct((2, 1, rows // 2), jnp.float32),
        jax.ShapeDtypeStruct((2, 1, rows // 2), jnp.float32),
        jax.ShapeDtypeStruct((2, width, rows // 2), jnp.float32),
    ]
    scratch = [pltpu.VMEM(s.shape, s.dtype) for s in shapes]
    result = jax.ShapeDtypeStruct((rows, width), queries.dtype)
    vmem = pl.BlockSpec(memory_space=pltpu.VMEM)
    smem = pl.BlockSpec(memory_space=pltpu.SMEM)

    def call(kernel, blocks, state, out_shape, tasks, scratch_shapes=()):
        inputs = [block_order, query, *blocks, *state]
        flops = 4 * tasks * groups * half * rows // 2 * width
        return pl.pallas_call(
            kernel,
            out_shape=out_shape,
            in_specs=[smem] + [vmem] * (len(inputs) - 1),
            out_specs=jax.tree.map(lambda _: vmem, out_shape),
            scratch_shapes=scratch_shapes,
            compiler_params=pltpu.CompilerParams(vmem_limit_bytes=16 * 2**20),
            cost_estimate=pl.CostEstimate(
                flops=flops, bytes_accessed=rows * width * 2, transcendentals=tasks * half * rows
            ),
        )(*inputs)

    def permute(value, pairs):
        return lax.ppermute(value, "seq", pairs)

    if devices == 4:
        first = permute(packed, [(0, 2), (3, 1), (1, 0), (2, 3)])
        second = permute(packed, [(1, 3), (2, 0), (0, 1), (3, 2)])
        inner = permute(packed, [(1, 2), (2, 1), (0, 0), (3, 3)])
        state = call(functools.partial(own_kernel, lanes, scale), [packed], [], shapes, 3)
        outer = permute(first, [(2, 3), (1, 0), (0, 1), (3, 2)])
        state = call(
            functools.partial(middle_kernel, lanes, scale, [(1, 3, 0, 2), (2, 0, 3, 1)]),
            [first, second],
            state,
            shapes,
            4,
        )
        out = call(
            functools.partial(
                last_kernel, lanes, scale, [(0, 2, 1, 3), (3, 0, 3, 0)], (1, 0, 0, 1)
            ),
            [inner, outer],
            state,
            result,
            2,
            scratch,
        )
    else:
        blocks = lax.all_gather(packed, "seq", axis=0, tiled=False)
        state = call(functools.partial(own_kernel, lanes, scale), [packed], [], shapes, 3)
        out = call(
            functools.partial(gathered_kernel, lanes, scale), [blocks], state, result, 2 * devices, scratch
        )
    return out.reshape(tokens, heads, width)


def solution(mesh):
    placed = (
        P(("grp", "seq"), "head", None),
        P(("grp", "seq"), "head", None),
        P(("grp", "seq"), "head", None),
        P("grp"),
    )
    return jax.shard_map(
        on_device,
        mesh=mesh,
        in_specs=placed,
        out_specs=P(("grp", "seq"), "head", None),
        check_vma=False,
    )
```

```python
import functools

import jax
import jax.numpy as jnp
from jax import lax
from jax.experimental import pallas as pl
from jax.experimental.pallas import tpu as pltpu
from jax.sharding import PartitionSpec as P

LOW = -1e30
LOG2E = 1.4426950408889634


def pick(table, index):
    value = jnp.int32(table[0])
    for place in range(1, len(table)):
        value = jnp.where(index == place, jnp.int32(table[place]), value)
    return value


def attend(query, blocks, lanes, scale, state, diagonal):
    groups, per_token = lanes
    rows = query.shape[0]
    keys = blocks[0][0].shape[0] // groups
    lane = lax.broadcasted_iota(jnp.int32, (keys, rows), 1)
    group = (lane % per_token) // (per_token // groups)
    parts = []
    for key, _ in blocks:
        both = lax.dot_general(
            key, query, (((1,), (1,)), ((), ())), preferred_element_type=jnp.float32
        )
        part = both[:keys]
        for g in range(1, groups):
            part = jnp.where(group == g, both[g * keys : (g + 1) * keys], part)
        part = part * scale
        if diagonal:
            place = lax.broadcasted_iota(jnp.int32, (keys, rows), 0)
            part = jnp.where(place <= lane // per_token, part, LOW)
        parts.append(part)
    top = functools.reduce(jnp.maximum, [jnp.max(part, axis=0, keepdims=True) for part in parts])
    if state is not None:
        top = jnp.maximum(top, state[0])
    total = 0.0
    spread = []
    for part in parts:
        weights = jnp.exp2(part - top)
        total = total + jnp.sum(weights, axis=0, keepdims=True)
        rounded = weights.astype(jnp.bfloat16)
        nothing = jnp.zeros_like(rounded)
        spread += [jnp.where(group == g, rounded, nothing) for g in range(groups)]
    product = lax.dot_general(
        jnp.concatenate([value for _, value in blocks], axis=0),
        jnp.concatenate(spread, axis=0),
        (((0,), (0,)), ((), ())),
        preferred_element_type=jnp.float32,
    )
    if state is None:
        return top, total, product
    factor = jnp.exp2(state[0] - top)
    return top, state[1] * factor + total, state[2] * factor + product


def load(refs, slot):
    return tuple(ref[slot] for ref in refs)


def store(refs, slot, state):
    for ref, part in zip(refs, state, strict=True):
        ref[slot] = part


def rows_of(ref, slot):
    half = ref.shape[0] // 2
    return ref[pl.ds(pl.multiple_of(slot * half, half), half), :]


def order_of(order, me, source):
    mine, theirs = order[2 * me], order[2 * source]
    mine_too, theirs_too = order[2 * me + 1], order[2 * source + 1]
    late = jnp.where(mine < mine_too, 1, 0)
    source_late = jnp.where(theirs < theirs_too, 1, 0)
    before = jnp.where(jnp.minimum(theirs, theirs_too) < jnp.minimum(mine, mine_too), 1, 0)
    return late + 2 * source_late + 4 * before


def own_kernel(lanes, scale, sources, order, query, packed, top, total, acc, codes):
    me = lax.axis_index("seq")
    refs = (top, total, acc)
    row = lax.broadcasted_iota(jnp.int32, codes.shape, 0)
    value = jnp.zeros(codes.shape, jnp.int32)
    for number, table in enumerate(sources):
        value = jnp.where(row == number, order_of(order, me, pick(table, me)), value)
    codes[...] = value
    late = jnp.where(order[2 * me] < order[2 * me + 1], 1, 0)
    for slot in range(2):
        block = (packed[slot, 0], packed[slot, 1])
        store(refs, slot, attend(rows_of(query, slot), [block], lanes, scale, None, True))
    block = (packed[1 - late, 0], packed[1 - late, 1])
    store(
        refs, late, attend(rows_of(query, late), [block], lanes, scale, load(refs, late), False)
    )


def split(code):
    return code % 2, (code // 2) % 2, code // 4


def code_of(codes, number):
    return codes[number : number + 1, 0:1][0, 0]


def remote(lanes, scale, code, query, packed, refs):
    late, source_late, before = split(code)
    mine = jnp.where(before == 1, 1 - late, late)
    theirs = jnp.where(before == 1, 1 - source_late, source_late)
    for slot, source_slot in ((mine, theirs), (late, 1 - source_late)):
        block = (packed[source_slot, 0], packed[source_slot, 1])
        state = attend(rows_of(query, slot), [block], lanes, scale, load(refs, slot), False)
        store(refs, slot, state)


def finish(state, staged, out, slot, done):
    result = state[2] * (1.0 / state[1])
    staged[slot] = result.astype(staged.dtype).T
    half = staged.shape[1]
    rows = pl.ds(pl.multiple_of(slot * half, half), half)
    pltpu.make_async_copy(staged.at[slot], out.at[rows], done.at[slot]).start()


def settle(staged, out, done):
    half = staged.shape[1]
    for slot in range(2):
        rows = pl.ds(slot * half, half)
        pltpu.make_async_copy(staged.at[slot], out.at[rows], done.at[slot]).wait()


def middle_kernel(lanes, scale, numbers, codes, query, *rest):
    blocks, before, refs = rest[: len(numbers)], rest[-6:-3], rest[-3:]
    for slot in range(2):
        store(refs, slot, load(before, slot))
    for number, packed in zip(numbers, blocks, strict=True):
        remote(lanes, scale, code_of(codes, number), query, packed, refs)


def last_kernel(lanes, scale, numbers, choose, codes, query, *rest):
    blocks = rest[: len(numbers)]
    refs, out, staged, done = rest[-6:-3], rest[-3], rest[-2], rest[-1]
    chosen = pick(choose, lax.axis_index("seq"))
    code = code_of(codes, numbers[0])
    for place in range(1, len(numbers)):
        code = jnp.where(chosen == place, code_of(codes, numbers[place]), code)

    def take(slot):
        parts = []
        for which in range(2):
            value = blocks[0][slot, which]
            for place in range(1, len(numbers)):
                value = jnp.where(chosen == place, blocks[place][slot, which], value)
            parts.append(value)
        return tuple(parts)

    late, source_late, before = split(code)
    early = 1 - late

    @pl.when(before == 1)
    def _():
        block = take(1 - source_late)
        for slot in (early, late):
            state = attend(rows_of(query, slot), [block], lanes, scale, load(refs, slot), False)
            finish(state, staged, out, slot, done)

    @pl.when(before == 0)
    def _():
        finish(load(refs, early), staged, out, early, done)
        pair = [take(0), take(1)]
        state = attend(rows_of(query, late), pair, lanes, scale, load(refs, late), False)
        finish(state, staged, out, late, done)

    settle(staged, out, done)


def gathered_kernel(lanes, scale, order, query, blocks, *rest):
    before, out, staged, done, refs = rest[:3], rest[3], rest[4], rest[5], rest[6:]
    me = lax.axis_index("seq")
    count = blocks.shape[0]
    for slot in range(2):
        store(refs, slot, load(before, slot))

    def step(index, carry):
        source = lax.rem(me + index, count)
        code = order_of(order, me, source)
        remote(lanes, scale, code, query, blocks.at[source], refs)
        return carry

    lax.fori_loop(1, count, step, 0)
    for slot in range(2):
        finish(load(refs, slot), staged, out, slot, done)
    settle(staged, out, done)


def on_device(queries, keys, values, block_order):
    tokens, heads, width = queries.shape
    groups = keys.shape[1]
    half = tokens // 2
    devices = lax.axis_size("seq")
    scale = width ** (-0.5) * LOG2E
    lanes = (groups, heads)
    rows = tokens * heads
    query = queries.reshape(rows, width)

    def pack(array):
        split = array.reshape(2, half, groups, width)
        return jnp.transpose(split, (0, 2, 1, 3)).reshape(2, 1, groups * half, width)

    packed = jnp.concatenate([pack(keys), pack(values)], axis=1)
    shapes = [
        jax.ShapeDtypeStruct((2, 1, rows // 2), jnp.float32),
        jax.ShapeDtypeStruct((2, 1, rows // 2), jnp.float32),
        jax.ShapeDtypeStruct((2, width, rows // 2), jnp.float32),
    ]
    result = jax.ShapeDtypeStruct((rows, width), queries.dtype)
    staging = [
        pltpu.VMEM((2, rows // 2, width), queries.dtype),
        pltpu.SemaphoreType.DMA((2,)),
    ]
    vmem = pl.BlockSpec(memory_space=pltpu.VMEM)
    smem = pl.BlockSpec(memory_space=pltpu.SMEM)
    anywhere = pl.BlockSpec(memory_space=pl.ANY)

    def call(kernel, tasks, first, blocks, state, out_shape, out_specs, scratch=(), first_spec=vmem):
        inputs = [first, query, *blocks, *state]
        return pl.pallas_call(
            functools.partial(kernel, lanes, scale),
            out_shape=out_shape,
            in_specs=[first_spec] + [vmem] * (len(inputs) - 1),
            out_specs=out_specs,
            scratch_shapes=scratch,
            compiler_params=pltpu.CompilerParams(vmem_limit_bytes=16 * 2**20),
            cost_estimate=pl.CostEstimate(
                flops=4 * tasks * groups * half * rows // 2 * width,
                bytes_accessed=rows * width * 2,
                transcendentals=tasks * half * rows,
            ),
        )(*inputs)

    def own(sources):
        codes = jax.ShapeDtypeStruct((8, 128), jnp.int32)

        def kernel(lanes, scale, *refs):
            own_kernel(lanes, scale, sources, *refs)

        return call(
            kernel, 3, block_order, [packed], [], [*shapes, codes], [vmem] * 4, first_spec=smem
        )

    def permute(value, pairs):
        return lax.ppermute(value, "seq", pairs)

    if devices == 4:
        first = permute(packed, [(0, 2), (3, 1), (1, 0), (2, 3)])
        second = permute(packed, [(1, 3), (2, 0), (0, 1), (3, 2)])
        inner = permute(packed, [(1, 2), (2, 1), (0, 0), (3, 3)])
        *state, codes = own([(1, 3, 0, 2), (2, 0, 3, 1), (0, 2, 1, 3), (3, 0, 3, 0)])
        outer = permute(first, [(2, 3), (1, 0), (0, 1), (3, 2)])

        def middle(lanes, scale, *refs):
            middle_kernel(lanes, scale, (0, 1), *refs)

        state = call(middle, 4, codes, [first, second], state, shapes, [vmem] * 3)

        def last(lanes, scale, *refs):
            last_kernel(lanes, scale, (2, 3), (1, 0, 0, 1), *refs)

        out = call(last, 2, codes, [inner, outer], state, result, anywhere, staging)
    else:
        blocks = lax.all_gather(packed, "seq", axis=0, tiled=False)
        *state, codes = own([])
        out = call(
            gathered_kernel,
            2 * devices,
            block_order,
            [blocks],
            state,
            result,
            anywhere,
            staging + [pltpu.VMEM(s.shape, s.dtype) for s in shapes],
            first_spec=smem,
        )
    return out.reshape(tokens, heads, width)


def solution(mesh):
    placed = (
        P(("grp", "seq"), "head", None),
        P(("grp", "seq"), "head", None),
        P(("grp", "seq"), "head", None),
        P("grp"),
    )
    return jax.shard_map(
        on_device,
        mesh=mesh,
        in_specs=placed,
        out_specs=P(("grp", "seq"), "head", None),
        check_vma=False,
    )
```

```python
import functools

import jax
import jax.numpy as jnp
from jax import lax
from jax.experimental import pallas as pl
from jax.experimental.pallas import tpu as pltpu
from jax.sharding import PartitionSpec as P

LOW = -1e30
LOG2E = 1.4426950408889634


def pick(table, index):
    value = jnp.int32(table[0])
    for place in range(1, len(table)):
        value = jnp.where(index == place, jnp.int32(table[place]), value)
    return value


def score(query, blocks, lanes, scale, diagonal):
    groups, per_token = lanes
    rows = query.shape[0]
    keys = blocks[0][0].shape[0] // groups
    lane = lax.broadcasted_iota(jnp.int32, (keys, rows), 1)
    group = (lane % per_token) // (per_token // groups)
    parts = []
    for key, _ in blocks:
        both = lax.dot_general(
            key, query, (((1,), (1,)), ((), ())), preferred_element_type=jnp.float32
        )
        part = both[:keys]
        for g in range(1, groups):
            part = jnp.where(group == g, both[g * keys : (g + 1) * keys], part)
        part = part * scale
        if diagonal:
            place = lax.broadcasted_iota(jnp.int32, (keys, rows), 0)
            part = jnp.where(place <= lane // per_token, part, LOW)
        parts.append(part)
    return parts


def weigh(parts, blocks, lanes, state):
    groups, per_token = lanes
    lane = lax.broadcasted_iota(jnp.int32, parts[0].shape, 1)
    group = (lane % per_token) // (per_token // groups)
    top = functools.reduce(jnp.maximum, [jnp.max(part, axis=0, keepdims=True) for part in parts])
    if state is not None:
        top = jnp.maximum(top, state[0])
    total = 0.0
    spread = []
    for part in parts:
        weights = jnp.exp2(part - top)
        total = total + jnp.sum(weights, axis=0, keepdims=True)
        rounded = weights.astype(jnp.bfloat16)
        nothing = jnp.zeros_like(rounded)
        spread += [jnp.where(group == g, rounded, nothing) for g in range(groups)]
    product = lax.dot_general(
        jnp.concatenate([value for _, value in blocks], axis=0),
        jnp.concatenate(spread, axis=0),
        (((0,), (0,)), ((), ())),
        preferred_element_type=jnp.float32,
    )
    if state is None:
        return top, total, product
    factor = jnp.exp2(state[0] - top)
    return top, state[1] * factor + total, state[2] * factor + product


def attend(query, blocks, lanes, scale, state, diagonal):
    return weigh(score(query, blocks, lanes, scale, diagonal), blocks, lanes, state)


def load(refs, slot):
    return tuple(ref[slot] for ref in refs)


def store(refs, slot, state):
    for ref, part in zip(refs, state, strict=True):
        ref[slot] = part


def rows_of(ref, slot):
    half = ref.shape[0] // 2
    return ref[pl.ds(pl.multiple_of(slot * half, half), half), :]


def order_of(order, me, source):
    mine, theirs = order[2 * me], order[2 * source]
    mine_too, theirs_too = order[2 * me + 1], order[2 * source + 1]
    late = jnp.where(mine < mine_too, 1, 0)
    source_late = jnp.where(theirs < theirs_too, 1, 0)
    before = jnp.where(jnp.minimum(theirs, theirs_too) < jnp.minimum(mine, mine_too), 1, 0)
    return late + 2 * source_late + 4 * before


def diagonal_kernel(lanes, scale, query, packed, *refs):
    blocks = [(packed[slot, 0], packed[slot, 1]) for slot in range(2)]
    queries = [rows_of(query, slot) for slot in range(2)]
    parts = [score(queries[slot], [blocks[slot]], lanes, scale, True) for slot in range(2)]
    for slot in range(2):
        store(refs, slot, weigh(parts[slot], [blocks[slot]], lanes, None))


def cross(lanes, scale, order, me, query, packed, before, refs):
    late = jnp.where(order[2 * me] < order[2 * me + 1], 1, 0)
    early = 1 - late
    store(refs, early, load(before, early))
    block = (packed[early, 0], packed[early, 1])
    state = attend(rows_of(query, late), [block], lanes, scale, load(before, late), False)
    store(refs, late, state)


def split(code):
    return code % 2, (code // 2) % 2, code // 4


def code_of(codes, number):
    return codes[number : number + 1, 0:1][0, 0]


def remote(lanes, scale, code, query, packed, refs):
    late, source_late, before = split(code)
    mine = jnp.where(before == 1, 1 - late, late)
    theirs = jnp.where(before == 1, 1 - source_late, source_late)
    for slot, source_slot in ((mine, theirs), (late, 1 - source_late)):
        block = (packed[source_slot, 0], packed[source_slot, 1])
        state = attend(rows_of(query, slot), [block], lanes, scale, load(refs, slot), False)
        store(refs, slot, state)


def finish(state, staged, out, slot, done):
    result = state[2] * (1.0 / state[1])
    staged[slot] = result.astype(staged.dtype).T
    half = staged.shape[1]
    rows = pl.ds(pl.multiple_of(slot * half, half), half)
    pltpu.make_async_copy(staged.at[slot], out.at[rows], done.at[slot]).start()


def settle(staged, out, done):
    half = staged.shape[1]
    for slot in range(2):
        rows = pl.ds(slot * half, half)
        pltpu.make_async_copy(staged.at[slot], out.at[rows], done.at[slot]).wait()


def middle_kernel(lanes, scale, sources, order, query, packed, *rest):
    count = len(rest) - 7
    blocks, before, refs, codes = rest[:count], rest[count : count + 3], rest[count + 3 : -1], rest[-1]
    me = lax.axis_index("seq")
    row = lax.broadcasted_iota(jnp.int32, codes.shape, 0)
    value = jnp.zeros(codes.shape, jnp.int32)
    numbers = [order_of(order, me, pick(table, me)) for table in sources]
    for place, number in enumerate(numbers):
        value = jnp.where(row == place, number, value)
    codes[...] = value
    cross(lanes, scale, order, me, query, packed, before, refs)
    for number, block in zip(numbers, blocks):
        remote(lanes, scale, number, query, block, refs)


def last_kernel(lanes, scale, numbers, choose, codes, query, *rest):
    blocks = rest[: len(numbers)]
    refs, out, staged, done = rest[-6:-3], rest[-3], rest[-2], rest[-1]
    chosen = pick(choose, lax.axis_index("seq"))
    code = code_of(codes, numbers[0])
    for place in range(1, len(numbers)):
        code = jnp.where(chosen == place, code_of(codes, numbers[place]), code)

    def take(slot):
        parts = []
        for which in range(2):
            value = blocks[0][slot, which]
            for place in range(1, len(numbers)):
                value = jnp.where(chosen == place, blocks[place][slot, which], value)
            parts.append(value)
        return tuple(parts)

    late, source_late, before = split(code)
    early = 1 - late

    @pl.when(before == 1)
    def _():
        block = take(1 - source_late)
        parts = [score(rows_of(query, slot), [block], lanes, scale, False) for slot in range(2)]
        states = [weigh(parts[slot], [block], lanes, load(refs, slot)) for slot in range(2)]
        for slot in range(2):
            finish(states[slot], staged, out, slot, done)

    @pl.when(before == 0)
    def _():
        finish(load(refs, early), staged, out, early, done)
        pair = [take(0), take(1)]
        state = attend(rows_of(query, late), pair, lanes, scale, load(refs, late), False)
        finish(state, staged, out, late, done)

    settle(staged, out, done)


def gathered_kernel(lanes, scale, order, query, packed, blocks, *rest):
    before, out, staged, done, refs = rest[:3], rest[3], rest[4], rest[5], rest[6:]
    me = lax.axis_index("seq")
    count = blocks.shape[0]
    cross(lanes, scale, order, me, query, packed, before, refs)

    def step(index, carry):
        source = lax.rem(me + index, count)
        code = order_of(order, me, source)
        remote(lanes, scale, code, query, blocks.at[source], refs)
        return carry

    lax.fori_loop(1, count, step, 0)
    for slot in range(2):
        finish(load(refs, slot), staged, out, slot, done)
    settle(staged, out, done)


def on_device(queries, keys, values, block_order):
    tokens, heads, width = queries.shape
    groups = keys.shape[1]
    half = tokens // 2
    devices = lax.axis_size("seq")
    scale = width ** (-0.5) * LOG2E
    lanes = (groups, heads)
    rows = tokens * heads
    query = queries.reshape(rows, width)

    def pack(array):
        split = array.reshape(2, half, groups, width)
        return jnp.transpose(split, (0, 2, 1, 3)).reshape(2, 1, groups * half, width)

    packed = jnp.concatenate([pack(keys), pack(values)], axis=1)
    shapes = [
        jax.ShapeDtypeStruct((2, 1, rows // 2), jnp.float32),
        jax.ShapeDtypeStruct((2, 1, rows // 2), jnp.float32),
        jax.ShapeDtypeStruct((2, width, rows // 2), jnp.float32),
    ]
    result = jax.ShapeDtypeStruct((rows, width), queries.dtype)
    staging = [
        pltpu.VMEM((2, rows // 2, width), queries.dtype),
        pltpu.SemaphoreType.DMA((2,)),
    ]
    vmem = pl.BlockSpec(memory_space=pltpu.VMEM)
    smem = pl.BlockSpec(memory_space=pltpu.SMEM)
    anywhere = pl.BlockSpec(memory_space=pl.ANY)

    def call(kernel, tasks, inputs, out_shape, out_specs, scratch=(), scalars=False):
        return pl.pallas_call(
            functools.partial(kernel, lanes, scale),
            out_shape=out_shape,
            in_specs=[smem if scalars else vmem] + [vmem] * (len(inputs) - 1),
            out_specs=out_specs,
            scratch_shapes=scratch,
            compiler_params=pltpu.CompilerParams(vmem_limit_bytes=16 * 2**20),
            cost_estimate=pl.CostEstimate(
                flops=4 * tasks * groups * half * rows // 2 * width,
                bytes_accessed=rows * width * 2,
                transcendentals=tasks * half * rows,
            ),
        )(*inputs)

    def permute(value, pairs):
        return lax.ppermute(value, "seq", pairs)

    if devices == 4:
        first = permute(packed, [(0, 2), (3, 1), (1, 0), (2, 3)])
        state = call(diagonal_kernel, 2, [query, packed], shapes, [vmem] * 3)
        packed, state = lax.optimization_barrier((packed, state))
        second = permute(packed, [(1, 3), (2, 0), (0, 1), (3, 2)])
        inner = permute(packed, [(1, 2), (2, 1), (0, 0), (3, 3)])
        outer = permute(first, [(2, 3), (1, 0), (0, 1), (3, 2)])

        def middle(lanes, scale, *refs):
            sources = [(1, 3, 0, 2), (2, 0, 3, 1), (0, 2, 1, 3), (3, 0, 3, 0)]
            middle_kernel(lanes, scale, sources, *refs)

        codes = jax.ShapeDtypeStruct((8, 128), jnp.int32)
        inputs = [block_order, query, packed, first, second, *state]
        *state, codes = call(middle, 5, inputs, [*shapes, codes], [vmem] * 4, scalars=True)

        def last(lanes, scale, *refs):
            last_kernel(lanes, scale, (2, 3), (1, 0, 0, 1), *refs)

        inputs = [codes, query, inner, outer, *state]
        out = call(last, 2, inputs, result, anywhere, staging)
    else:
        blocks = lax.all_gather(packed, "seq", axis=0, tiled=False)
        state = call(diagonal_kernel, 2, [query, packed], shapes, [vmem] * 3)
        inputs = [block_order, query, packed, blocks, *state]
        scratch = staging + [pltpu.VMEM(s.shape, s.dtype) for s in shapes]
        out = call(gathered_kernel, 2 * devices, inputs, result, anywhere, scratch, scalars=True)
    return out.reshape(tokens, heads, width)


def solution(mesh):
    placed = (
        P(("grp", "seq"), "head", None),
        P(("grp", "seq"), "head", None),
        P(("grp", "seq"), "head", None),
        P("grp"),
    )
    return jax.shard_map(
        on_device,
        mesh=mesh,
        in_specs=placed,
        out_specs=P(("grp", "seq"), "head", None),
        check_vma=False,
    )
```

```python
import functools

import jax
import jax.numpy as jnp
from jax import lax
from jax.experimental import pallas as pl
from jax.experimental.pallas import tpu as pltpu
from jax.sharding import PartitionSpec as P


ROUTE = (
    ("o1", "packed", ((0, 2), (3, 1), (1, 0), (2, 3))),
    ("o2", "packed", ((1, 3), (2, 0), (0, 1), (3, 2))),
    ("x", "packed:0", ((0, 3), (3, 0), (1, 2), (2, 1))),
    ("z", "o1:1", ((0, 1), (1, 0), (2, 3), (3, 2))),
    ("y", "packed:1", ((1, 2), (2, 1), (0, 0), (3, 3))),
)
SOURCES = (
    ((("o1",),), (0, 0, 0, 0)),
    ((("o2",),), (0, 0, 0, 0)),
    ((("x", "z"), ("x", "y")), (0, 1, 1, 0)),
)
LOW = -1e30
LOG2E = 1.4426950408889634


def pick(table, index):
    value = jnp.int32(table[0])
    for place in range(1, len(table)):
        value = jnp.where(index == place, jnp.int32(table[place]), value)
    return value


def score(query, blocks, lanes, scale, diagonal):
    groups, per_token = lanes
    rows = query.shape[0]
    keys = blocks[0][0].shape[0] // groups
    lane = lax.broadcasted_iota(jnp.int32, (keys, rows), 1)
    group = (lane % per_token) // (per_token // groups)
    parts = []
    for key, _ in blocks:
        both = lax.dot_general(
            key, query, (((1,), (1,)), ((), ())), preferred_element_type=jnp.float32
        )
        part = both[:keys]
        for g in range(1, groups):
            part = jnp.where(group == g, both[g * keys : (g + 1) * keys], part)
        part = part * scale
        if diagonal:
            place = lax.broadcasted_iota(jnp.int32, (keys, rows), 0)
            part = jnp.where(place <= lane // per_token, part, LOW)
        parts.append(part)
    return parts


def weigh(parts, blocks, lanes, state):
    groups, per_token = lanes
    lane = lax.broadcasted_iota(jnp.int32, parts[0].shape, 1)
    group = (lane % per_token) // (per_token // groups)
    top = functools.reduce(jnp.maximum, [jnp.max(part, axis=0, keepdims=True) for part in parts])
    if state is not None:
        top = jnp.maximum(top, state[0])
    total = 0.0
    spread = []
    for part in parts:
        weights = jnp.exp2(part - top)
        total = total + jnp.sum(weights, axis=0, keepdims=True)
        rounded = weights.astype(jnp.bfloat16)
        nothing = jnp.zeros_like(rounded)
        spread += [jnp.where(group == g, rounded, nothing) for g in range(groups)]
    product = lax.dot_general(
        jnp.concatenate([value for _, value in blocks], axis=0),
        jnp.concatenate(spread, axis=0),
        (((0,), (0,)), ((), ())),
        preferred_element_type=jnp.float32,
    )
    if state is None:
        return top, total, product
    factor = jnp.exp2(state[0] - top)
    return top, state[1] * factor + total, state[2] * factor + product


def attend(query, blocks, lanes, scale, state, diagonal):
    return weigh(score(query, blocks, lanes, scale, diagonal), blocks, lanes, state)


def load(refs, slot):
    return tuple(ref[slot] for ref in refs)


def store(refs, slot, state):
    for ref, part in zip(refs, state, strict=True):
        ref[slot] = part


def rows_of(ref, slot):
    half = ref.shape[0] // 2
    return ref[pl.ds(pl.multiple_of(slot * half, half), half), :]


def order_of(order, me, source):
    mine, theirs = order[2 * me], order[2 * source]
    mine_too, theirs_too = order[2 * me + 1], order[2 * source + 1]
    late = jnp.where(mine < mine_too, 1, 0)
    source_late = jnp.where(theirs < theirs_too, 1, 0)
    before = jnp.where(jnp.minimum(theirs, theirs_too) < jnp.minimum(mine, mine_too), 1, 0)
    return late + 2 * source_late + 4 * before


def diagonal_kernel(lanes, scale, sources, order, query, packed, top, total, acc, codes, known, arrived):
    copy = pltpu.make_async_copy(order, known, arrived)
    copy.start()
    blocks = [(packed[slot, 0], packed[slot, 1]) for slot in range(2)]
    queries = [rows_of(query, slot) for slot in range(2)]
    parts = [score(queries[slot], [blocks[slot]], lanes, scale, True) for slot in range(2)]
    for slot in range(2):
        store((top, total, acc), slot, weigh(parts[slot], [blocks[slot]], lanes, None))
    copy.wait()
    me = lax.axis_index("seq")
    row = lax.broadcasted_iota(jnp.int32, codes.shape, 0)
    value = jnp.zeros(codes.shape, jnp.int32)
    for place, table in enumerate(sources):
        value = jnp.where(row == place, order_of(known, me, pick(table, me)), value)
    codes[...] = value


def split(code):
    return code % 2, (code // 2) % 2, code // 4


def code_of(codes, number):
    return codes[number : number + 1, 0:1][0, 0]


def fetch(option, slot, which):
    if len(option) == 1:
        return option[0][slot, which]
    if isinstance(slot, int):
        return option[slot][0, which]
    return jnp.where(slot == 0, option[0][0, which], option[1][0, which])


def chooser(options, chosen):
    def take(slot):
        parts = []
        for which in range(2):
            value = fetch(options[0], slot, which)
            for place in range(1, len(options)):
                value = jnp.where(chosen == place, fetch(options[place], slot, which), value)
            parts.append(value)
        return tuple(parts)

    return take


def group(refs, shape):
    options = []
    for length in shape:
        options.append(refs[:length])
        refs = refs[length:]
    return options


def remote(lanes, scale, code, query, take, extra, refs, emit):
    late, source_late, before = split(code)
    early = 1 - late
    more = [extra(early)] if extra else []

    @pl.when(before == 1)
    def _():
        block = take(1 - source_late)
        early_parts = score(rows_of(query, early), [block], lanes, scale, False)
        late_parts = score(rows_of(query, late), [block, *more], lanes, scale, False)
        early_state = weigh(early_parts, [block], lanes, load(refs, early))
        late_state = weigh(late_parts, [block, *more], lanes, load(refs, late))
        emit(early, early_state)
        emit(late, late_state)

    @pl.when(before == 0)
    def _():
        emit(early, load(refs, early))
        blocks = [take(0), take(1), *more]
        emit(late, attend(rows_of(query, late), blocks, lanes, scale, load(refs, late), False))


def finish(state, staged, out, slot, done):
    result = state[2] * (1.0 / state[1])
    staged[slot] = result.astype(staged.dtype).T
    half = staged.shape[1]
    rows = pl.ds(pl.multiple_of(slot * half, half), half)
    pltpu.make_async_copy(staged.at[slot], out.at[rows], done.at[slot]).start()


def settle(staged, out, done):
    half = staged.shape[1]
    for slot in range(2):
        rows = pl.ds(slot * half, half)
        pltpu.make_async_copy(staged.at[slot], out.at[rows], done.at[slot]).wait()


def stage_kernel(lanes, scale, number, shape, choose, first, codes, query, *rest):
    blocks, before, after = rest[:-6], rest[-6:-3], rest[-3:]
    extra = None
    if first:
        own, blocks = blocks[0], blocks[1:]

        def extra(early):
            return own[early, 0], own[early, 1]

    take = chooser(group(blocks, shape), pick(choose, lax.axis_index("seq")))

    def emit(slot, state):
        store(after, slot, state)

    remote(lanes, scale, code_of(codes, number), query, take, extra, before, emit)


def last_kernel(lanes, scale, number, shape, choose, codes, query, *rest):
    blocks, before, out, staged, done = rest[:-6], rest[-6:-3], rest[-3], rest[-2], rest[-1]
    take = chooser(group(blocks, shape), pick(choose, lax.axis_index("seq")))

    def emit(slot, state):
        finish(state, staged, out, slot, done)

    remote(lanes, scale, code_of(codes, number), query, take, None, before, emit)
    settle(staged, out, done)


def gathered_kernel(lanes, scale, order, query, packed, blocks, *rest):
    before, out, staged, done, refs = rest[:3], rest[3], rest[4], rest[5], rest[6:]
    me = lax.axis_index("seq")
    count = blocks.shape[0]
    late = jnp.where(order[2 * me] < order[2 * me + 1], 1, 0)
    early = 1 - late
    store(refs, early, load(before, early))
    own = (packed[early, 0], packed[early, 1])
    store(refs, late, attend(rows_of(query, late), [own], lanes, scale, load(before, late), False))

    def emit(slot, state):
        store(refs, slot, state)

    def step(index, carry):
        source = lax.rem(me + index, count)
        take = chooser([[blocks.at[source]]], 0)
        remote(lanes, scale, order_of(order, me, source), query, take, None, refs, emit)
        return carry

    lax.fori_loop(1, count, step, 0)
    for slot in range(2):
        finish(load(refs, slot), staged, out, slot, done)
    settle(staged, out, done)


def on_device(queries, keys, values, block_order):
    tokens, heads, width = queries.shape
    groups = keys.shape[1]
    half = tokens // 2
    devices = lax.axis_size("seq")
    scale = width ** (-0.5) * LOG2E
    lanes = (groups, heads)
    rows = tokens * heads
    query = queries.reshape(rows, width)

    def pack(array):
        split = array.reshape(2, half, groups, width)
        return jnp.transpose(split, (0, 2, 1, 3)).reshape(2, 1, groups * half, width)

    packed = jnp.concatenate([pack(keys), pack(values)], axis=1)
    shapes = [
        jax.ShapeDtypeStruct((2, 1, rows // 2), jnp.float32),
        jax.ShapeDtypeStruct((2, 1, rows // 2), jnp.float32),
        jax.ShapeDtypeStruct((2, width, rows // 2), jnp.float32),
    ]
    result = jax.ShapeDtypeStruct((rows, width), queries.dtype)
    staging = [
        pltpu.VMEM((2, rows // 2, width), queries.dtype),
        pltpu.SemaphoreType.DMA((2,)),
    ]
    vmem = pl.BlockSpec(memory_space=pltpu.VMEM)
    smem = pl.BlockSpec(memory_space=pltpu.SMEM)
    anywhere = pl.BlockSpec(memory_space=pl.ANY)

    def call(kernel, tasks, inputs, specs, out_shape, out_specs, scratch=()):
        return pl.pallas_call(
            functools.partial(kernel, lanes, scale),
            out_shape=out_shape,
            in_specs=specs + [vmem] * (len(inputs) - len(specs)),
            out_specs=out_specs,
            scratch_shapes=scratch,
            compiler_params=pltpu.CompilerParams(vmem_limit_bytes=16 * 2**20),
            cost_estimate=pl.CostEstimate(
                flops=4 * tasks * groups * half * rows // 2 * width,
                bytes_accessed=rows * width * 2,
                transcendentals=tasks * half * rows,
            ),
        )(*inputs)

    def diagonal(sources):
        def kernel(lanes, scale, *refs):
            diagonal_kernel(lanes, scale, sources, *refs)

        codes = jax.ShapeDtypeStruct((8, 128), jnp.int32)
        scratch = [pltpu.SMEM(block_order.shape, jnp.int32), pltpu.SemaphoreType.DMA]
        inputs = [block_order, query, packed]
        return call(kernel, 2, inputs, [anywhere], [*shapes, codes], [vmem] * 4, scratch)

    if devices == len(ROUTE[0][2]):
        held = {"packed": tuple(range(devices))}
        for name, sent, pairs in ROUTE:
            source = dict((target, origin) for origin, target in pairs)
            held[name] = tuple(held[sent.partition(":")[0]][source[i]] for i in range(devices))
        tables = [
            tuple(held[options[choose[i]][0]][i] for i in range(devices))
            for options, choose in SOURCES
        ]
        got = {"packed": packed}
        for name, sent, pairs in ROUTE:
            base, _, half_of = sent.partition(":")
            value = got[base]
            if half_of:
                value = value[int(half_of) : int(half_of) + 1]
            got[name] = lax.ppermute(value, "seq", pairs)
        *state, codes = diagonal(tables)
        final = len(SOURCES) - 1
        for stage, (options, choose) in enumerate(SOURCES[:final]):
            buffers = [got[name] for option in options for name in option]
            if stage == 0:
                buffers = [packed, *buffers]
            form = (stage, tuple(map(len, options)), choose, stage == 0)

            def kernel(lanes, scale, *refs, form=form):
                stage_kernel(lanes, scale, *form, *refs)

            inputs = [codes, query, *buffers, *state]
            state = call(kernel, 3, inputs, [], shapes, [vmem] * 3)

        options, choose = SOURCES[final]
        form = (final, tuple(map(len, options)), choose)

        def kernel(lanes, scale, *refs):
            last_kernel(lanes, scale, *form, *refs)

        inputs = [codes, query, *[got[name] for option in options for name in option], *state]
        out = call(kernel, 2, inputs, [], result, anywhere, staging)
    else:
        blocks = lax.all_gather(packed, "seq", axis=0, tiled=False)
        *state, _ = diagonal([])
        inputs = [block_order, query, packed, blocks, *state]
        scratch = staging + [pltpu.VMEM(s.shape, s.dtype) for s in shapes]
        out = call(gathered_kernel, 2 * devices, inputs, [smem], result, anywhere, scratch)
    return out.reshape(tokens, heads, width)


def solution(mesh):
    placed = (
        P(("grp", "seq"), "head", None),
        P(("grp", "seq"), "head", None),
        P(("grp", "seq"), "head", None),
        P("grp"),
    )

    return jax.shard_map(
        on_device,
        mesh=mesh,
        in_specs=placed,
        out_specs=P(("grp", "seq"), "head", None),
        check_vma=False,
    )
```

```python
import functools

import jax
import jax.numpy as jnp
from jax import lax
from jax.experimental import pallas as pl
from jax.experimental.pallas import tpu as pltpu
from jax.sharding import PartitionSpec as P


ROUTE = (
    ("o1", "packed", ((0, 2), (3, 1), (1, 0), (2, 3))),
    ("o2", "packed", ((1, 3), (2, 0), (0, 1), (3, 2))),
    ("x", "keys", ((0, 3), (3, 0), (1, 2), (2, 1))),
    ("z", "o1", ((0, 1), (1, 0), (2, 3), (3, 2))),
    ("y", "values", ((1, 2), (2, 1), (0, 0), (3, 3))),
)
WHOLE = ("o1", "o2")
LAST_KEYS = "x"
LAST_VALUES = ("z", "y")
CHOICE = (0, 1, 1, 0)
LOW = -1e30
LOG2E = 1.4426950408889634


def pick(table, index):
    value = jnp.int32(table[0])
    for place in range(1, len(table)):
        value = jnp.where(index == place, jnp.int32(table[place]), value)
    return value


def score(query, blocks, lanes, scale, diagonal):
    groups, per_token = lanes
    rows = query.shape[0]
    keys = blocks[0][0].shape[0] // groups
    lane = lax.broadcasted_iota(jnp.int32, (keys, rows), 1)
    group = (lane % per_token) // (per_token // groups)
    parts = []
    for key, _ in blocks:
        both = lax.dot_general(
            key, query, (((1,), (1,)), ((), ())), preferred_element_type=jnp.float32
        )
        part = both[:keys]
        for g in range(1, groups):
            part = jnp.where(group == g, both[g * keys : (g + 1) * keys], part)
        part = part * scale
        if diagonal:
            place = lax.broadcasted_iota(jnp.int32, (keys, rows), 0)
            part = jnp.where(place <= lane // per_token, part, LOW)
        parts.append(part)
    return parts


def soften(parts, lanes, state):
    groups, per_token = lanes
    lane = lax.broadcasted_iota(jnp.int32, parts[0].shape, 1)
    group = (lane % per_token) // (per_token // groups)
    top = functools.reduce(jnp.maximum, [jnp.max(part, axis=0, keepdims=True) for part in parts])
    if state is not None:
        top = jnp.maximum(top, state[0])
    total = 0.0
    spread = []
    for part in parts:
        weights = jnp.exp2(part - top)
        total = total + jnp.sum(weights, axis=0, keepdims=True)
        rounded = weights.astype(jnp.bfloat16)
        nothing = jnp.zeros_like(rounded)
        spread += [jnp.where(group == g, rounded, nothing) for g in range(groups)]
    factor = None
    if state is not None:
        factor = jnp.exp2(state[0] - top)
        total = state[1] * factor + total
    return top, total, factor, jnp.concatenate(spread, axis=0)


def multiply(value, spread):
    return lax.dot_general(
        value, spread, (((0,), (0,)), ((), ())), preferred_element_type=jnp.float32
    )


def weigh(parts, blocks, lanes, state):
    top, total, factor, spread = soften(parts, lanes, state)
    product = multiply(jnp.concatenate([value for _, value in blocks], axis=0), spread)
    if state is None:
        return top, total, product
    return top, total, state[2] * factor + product


def attend(query, blocks, lanes, scale, state, diagonal):
    return weigh(score(query, blocks, lanes, scale, diagonal), blocks, lanes, state)


def load(refs, slot):
    return tuple(ref[slot] for ref in refs)


def store(refs, slot, state):
    for ref, part in zip(refs, state, strict=True):
        ref[slot] = part


def rows_of(ref, slot):
    half = ref.shape[0] // 2
    return ref[pl.ds(pl.multiple_of(slot * half, half), half), :]


def order_of(order, me, source):
    mine, theirs = order[2 * me], order[2 * source]
    mine_too, theirs_too = order[2 * me + 1], order[2 * source + 1]
    late = jnp.where(mine < mine_too, 1, 0)
    source_late = jnp.where(theirs < theirs_too, 1, 0)
    before = jnp.where(jnp.minimum(theirs, theirs_too) < jnp.minimum(mine, mine_too), 1, 0)
    return late + 2 * source_late + 4 * before


def diagonal_kernel(lanes, scale, sources, order, query, packed, top, total, acc, codes, known, arrived):
    copy = pltpu.make_async_copy(order, known, arrived)
    copy.start()
    blocks = [(packed[slot, 0], packed[slot, 1]) for slot in range(2)]
    queries = [rows_of(query, slot) for slot in range(2)]
    parts = [score(queries[slot], [blocks[slot]], lanes, scale, True) for slot in range(2)]
    for slot in range(2):
        store((top, total, acc), slot, weigh(parts[slot], [blocks[slot]], lanes, None))
    copy.wait()
    me = lax.axis_index("seq")
    row = lax.broadcasted_iota(jnp.int32, codes.shape, 0)
    value = jnp.zeros(codes.shape, jnp.int32)
    for place, table in enumerate(sources):
        value = jnp.where(row == place, order_of(known, me, pick(table, me)), value)
    codes[...] = value


def split(code):
    return code % 2, (code // 2) % 2, code // 4


def code_of(codes, number):
    return codes[number : number + 1, 0:1][0, 0]


def remote(lanes, scale, code, query, take, extra, refs, emit):
    late, source_late, before = split(code)
    early = 1 - late
    more = [extra(early)] if extra else []

    @pl.when(before == 1)
    def _():
        block = take(1 - source_late)
        early_parts = score(rows_of(query, early), [block], lanes, scale, False)
        late_parts = score(rows_of(query, late), [block, *more], lanes, scale, False)
        early_state = weigh(early_parts, [block], lanes, load(refs, early))
        late_state = weigh(late_parts, [block, *more], lanes, load(refs, late))
        emit(early, early_state)
        emit(late, late_state)

    @pl.when(before == 0)
    def _():
        emit(early, load(refs, early))
        blocks = [take(0), take(1), *more]
        emit(late, attend(rows_of(query, late), blocks, lanes, scale, load(refs, late), False))


def finish(result, staged, out, slot, done):
    staged[slot] = result.astype(staged.dtype).T
    half = staged.shape[1]
    rows = pl.ds(pl.multiple_of(slot * half, half), half)
    pltpu.make_async_copy(staged.at[slot], out.at[rows], done.at[slot]).start()


def settle(staged, out, done):
    half = staged.shape[1]
    for slot in range(2):
        rows = pl.ds(slot * half, half)
        pltpu.make_async_copy(staged.at[slot], out.at[rows], done.at[slot]).wait()


def block_of(packed):
    return lambda slot: (packed[slot, 0], packed[slot, 1])


def stage_kernel(number, lanes, scale, codes, query, *rest):
    blocks, before, after = rest[:-6], rest[-6:-3], rest[-3:]
    extra = block_of(blocks[1]) if len(blocks) > 1 else None

    def emit(slot, state):
        store(after, slot, state)

    code = code_of(codes, number)
    remote(lanes, scale, code, query, block_of(blocks[0]), extra, before, emit)


def weights_kernel(number, lanes, scale, codes, query, keys, top, total, acc, spread, share, base):
    refs = (top, total, acc)
    late, source_late, before = split(code_of(codes, number))
    early = 1 - late

    @pl.when(before == 1)
    def _():
        block = (keys[1 - source_late, 0], None)
        parts = [score(rows_of(query, slot), [block], lanes, scale, False) for slot in range(2)]
        for slot in range(2):
            _, new_total, factor, weights = soften(parts[slot], lanes, load(refs, slot))
            inverse = 1.0 / new_total
            spread[slot] = weights
            share[slot] = inverse
            base[slot] = acc[slot] * (factor * inverse)

    @pl.when(before == 0)
    def _():
        blocks = [(keys[slot, 0], None) for slot in range(2)]
        parts = score(rows_of(query, late), blocks, lanes, scale, False)
        _, new_total, factor, weights = soften(parts, lanes, load(refs, late))
        inverse = 1.0 / new_total
        half = weights.shape[0] // 2
        spread[0] = weights[:half]
        spread[1] = weights[half:]
        share[late] = inverse
        base[late] = acc[late] * (factor * inverse)
        base[early] = acc[early] * (1.0 / total[early])


def values_kernel(number, lanes, scale, codes, near, far, spread, share, base, out, staged, done):
    chosen = pick(CHOICE, lax.axis_index("seq"))
    late, source_late, before = split(code_of(codes, number))

    def take(slot):
        return jnp.where(chosen == 0, near[slot, 0], far[slot, 0])

    @pl.when(before == 1)
    def _():
        value = take(1 - source_late)
        products = [multiply(value, spread[slot]) for slot in range(2)]
        for slot in range(2):
            finish(base[slot] + products[slot] * share[slot], staged, out, slot, done)

    @pl.when(before == 0)
    def _():
        finish(base[1 - late], staged, out, 1 - late, done)
        value = jnp.concatenate([take(0), take(1)], axis=0)
        product = multiply(value, jnp.concatenate([spread[0], spread[1]], axis=0))
        finish(base[late] + product * share[late], staged, out, late, done)

    settle(staged, out, done)


def gathered_kernel(lanes, scale, order, query, packed, blocks, *rest):
    before, out, staged, done, refs = rest[:3], rest[3], rest[4], rest[5], rest[6:]
    me = lax.axis_index("seq")
    count = blocks.shape[0]
    late = jnp.where(order[2 * me] < order[2 * me + 1], 1, 0)
    early = 1 - late
    store(refs, early, load(before, early))
    own = (packed[early, 0], packed[early, 1])
    store(refs, late, attend(rows_of(query, late), [own], lanes, scale, load(before, late), False))

    def emit(slot, state):
        store(refs, slot, state)

    def step(index, carry):
        source = lax.rem(me + index, count)
        take = block_of(blocks.at[source])
        remote(lanes, scale, order_of(order, me, source), query, take, None, refs, emit)
        return carry

    lax.fori_loop(1, count, step, 0)
    _, total, acc = refs
    for slot in range(2):
        finish(acc[slot] * (1.0 / total[slot]), staged, out, slot, done)
    settle(staged, out, done)


def on_device(queries, keys, values, block_order):
    tokens, heads, width = queries.shape
    groups = keys.shape[1]
    half = tokens // 2
    devices = lax.axis_size("seq")
    scale = width ** (-0.5) * LOG2E
    lanes = (groups, heads)
    rows = tokens * heads
    query = queries.reshape(rows, width)

    def pack(array):
        split = array.reshape(2, half, groups, width)
        return jnp.transpose(split, (0, 2, 1, 3)).reshape(2, 1, groups * half, width)

    halves = {"keys": pack(keys), "values": pack(values)}
    packed = jnp.concatenate([halves["keys"], halves["values"]], axis=1)
    shapes = [
        jax.ShapeDtypeStruct((2, 1, rows // 2), jnp.float32),
        jax.ShapeDtypeStruct((2, 1, rows // 2), jnp.float32),
        jax.ShapeDtypeStruct((2, width, rows // 2), jnp.float32),
    ]
    result = jax.ShapeDtypeStruct((rows, width), queries.dtype)
    staging = [
        pltpu.VMEM((2, rows // 2, width), queries.dtype),
        pltpu.SemaphoreType.DMA((2,)),
    ]
    vmem = pl.BlockSpec(memory_space=pltpu.VMEM)
    smem = pl.BlockSpec(memory_space=pltpu.SMEM)
    anywhere = pl.BlockSpec(memory_space=pl.ANY)

    def call(kernel, tasks, inputs, specs, out_shape, out_specs, scratch=()):
        return pl.pallas_call(
            functools.partial(kernel, lanes, scale),
            out_shape=out_shape,
            in_specs=specs + [vmem] * (len(inputs) - len(specs)),
            out_specs=out_specs,
            scratch_shapes=scratch,
            compiler_params=pltpu.CompilerParams(vmem_limit_bytes=16 * 2**20),
            cost_estimate=pl.CostEstimate(
                flops=4 * tasks * groups * half * rows // 2 * width,
                bytes_accessed=rows * width * 2,
                transcendentals=tasks * half * rows,
            ),
        )(*inputs)

    def diagonal(sources):
        def kernel(lanes, scale, *refs):
            diagonal_kernel(lanes, scale, sources, *refs)

        codes = jax.ShapeDtypeStruct((8, 128), jnp.int32)
        scratch = [pltpu.SMEM(block_order.shape, jnp.int32), pltpu.SemaphoreType.DMA]
        inputs = [block_order, query, packed]
        return call(kernel, 2, inputs, [anywhere], [*shapes, codes], [vmem] * 4, scratch)

    if devices == len(CHOICE):
        mine = tuple(range(devices))
        held = {name: mine for name in ("packed", *halves)}
        got = {"packed": packed, **halves}
        for name, sent, pairs in ROUTE:
            source = dict((target, origin) for origin, target in pairs)
            held[name] = tuple(held[sent][source[i]] for i in range(devices))
            value = got[sent]
            if name in LAST_VALUES and value.shape[1] > 1:
                value = value[:, 1:]
            got[name] = lax.ppermute(value, "seq", pairs)
        *state, codes = diagonal([held[name] for name in (*WHOLE, LAST_KEYS)])
        for stage, name in enumerate(WHOLE):
            blocks = [got[name]] if stage else [got[name], packed]
            kernel = functools.partial(stage_kernel, stage)
            inputs = [codes, query, *blocks, *state]
            state = call(kernel, 3, inputs, [], shapes, [vmem] * 3)
        kernel = functools.partial(weights_kernel, len(WHOLE))
        spread = jax.ShapeDtypeStruct((2, groups * half, rows // 2), jnp.bfloat16)
        inputs = [codes, query, got[LAST_KEYS], *state]
        state = call(kernel, 1, inputs, [], [spread, *shapes[1:]], [vmem] * 3)
        kernel = functools.partial(values_kernel, len(WHOLE))
        inputs = [codes, *[got[name] for name in LAST_VALUES], *state]
        out = call(kernel, 1, inputs, [], result, anywhere, staging)
    else:
        blocks = lax.all_gather(packed, "seq", axis=0, tiled=False)
        *state, _ = diagonal([])
        inputs = [block_order, query, packed, blocks, *state]
        scratch = staging + [pltpu.VMEM(s.shape, s.dtype) for s in shapes]
        out = call(gathered_kernel, 2 * devices, inputs, [smem], result, anywhere, scratch)
    return out.reshape(tokens, heads, width)


def solution(mesh):
    placed = (
        P(("grp", "seq"), "head", None),
        P(("grp", "seq"), "head", None),
        P(("grp", "seq"), "head", None),
        P("grp"),
    )

    return jax.shard_map(
        on_device,
        mesh=mesh,
        in_specs=placed,
        out_specs=P(("grp", "seq"), "head", None),
        check_vma=False,
    )
```

```python
import functools

import jax
import jax.numpy as jnp
from jax import lax
from jax.experimental import pallas as pl
from jax.experimental.pallas import tpu as pltpu
from jax.sharding import PartitionSpec as P


ROUTE = (
    ("o1", "packed", ((0, 2), (3, 1), (1, 0), (2, 3))),
    ("o2", "packed", ((1, 3), (2, 0), (0, 1), (3, 2))),
    ("x", "keys", ((0, 3), (3, 0), (1, 2), (2, 1))),
    ("z", "o1", ((0, 1), (1, 0), (2, 3), (3, 2))),
    ("y", "values", ((1, 2), (2, 1), (0, 0), (3, 3))),
)
WHOLE = ("o1", "o2")
LAST_KEYS = "x"
LAST_VALUES = ("z", "y")
CHOICE = (0, 1, 1, 0)
LOW = -1e30
LOG2E = 1.4426950408889634


def pick(table, index):
    value = jnp.int32(table[0])
    for place in range(1, len(table)):
        value = jnp.where(index == place, jnp.int32(table[place]), value)
    return value


def score(query, blocks, lanes, scale, diagonal):
    groups, per_token = lanes
    rows = query.shape[0]
    keys = blocks[0][0].shape[0] // groups
    lane = lax.broadcasted_iota(jnp.int32, (keys, rows), 1)
    group = (lane % per_token) // (per_token // groups)
    parts = []
    for key, _ in blocks:
        both = lax.dot_general(
            key, query, (((1,), (1,)), ((), ())), preferred_element_type=jnp.float32
        )
        part = both[:keys]
        for g in range(1, groups):
            part = jnp.where(group == g, both[g * keys : (g + 1) * keys], part)
        part = part * scale
        if diagonal:
            place = lax.broadcasted_iota(jnp.int32, (keys, rows), 0)
            part = jnp.where(place <= lane // per_token, part, LOW)
        parts.append(part)
    return parts


def soften(parts, lanes, state, divide=False):
    groups, per_token = lanes
    lane = lax.broadcasted_iota(jnp.int32, parts[0].shape, 1)
    group = (lane % per_token) // (per_token // groups)
    top = functools.reduce(jnp.maximum, [jnp.max(part, axis=0, keepdims=True) for part in parts])
    if state is not None:
        top = jnp.maximum(top, state[0])
    parts = [jnp.exp2(part - top) for part in parts]
    total = sum(jnp.sum(weights, axis=0, keepdims=True) for weights in parts)
    factor = None
    if state is not None:
        factor = jnp.exp2(state[0] - top)
        total = state[1] * factor + total
    if divide:
        inverse = 1.0 / total
        factor = factor * inverse
        parts = [weights * inverse for weights in parts]
    spread = []
    for weights in parts:
        rounded = weights.astype(jnp.bfloat16)
        nothing = jnp.zeros_like(rounded)
        spread += [jnp.where(group == g, rounded, nothing) for g in range(groups)]
    return top, total, factor, jnp.concatenate(spread, axis=0)


def multiply(value, spread):
    return lax.dot_general(
        value, spread, (((0,), (0,)), ((), ())), preferred_element_type=jnp.float32
    )


def weigh(parts, blocks, lanes, state):
    top, total, factor, spread = soften(parts, lanes, state)
    product = multiply(jnp.concatenate([value for _, value in blocks], axis=0), spread)
    if state is None:
        return top, total, product
    return top, total, state[2] * factor + product


def attend(query, blocks, lanes, scale, state, diagonal):
    return weigh(score(query, blocks, lanes, scale, diagonal), blocks, lanes, state)


def load(refs, slot):
    return tuple(ref[slot] for ref in refs)


def store(refs, slot, state):
    for ref, part in zip(refs, state, strict=True):
        ref[slot] = part


def rows_of(ref, slot):
    half = ref.shape[0] // 2
    return ref[pl.ds(pl.multiple_of(slot * half, half), half), :]


def order_of(order, me, source):
    mine, theirs = order[2 * me], order[2 * source]
    mine_too, theirs_too = order[2 * me + 1], order[2 * source + 1]
    late = jnp.where(mine < mine_too, 1, 0)
    source_late = jnp.where(theirs < theirs_too, 1, 0)
    before = jnp.where(jnp.minimum(theirs, theirs_too) < jnp.minimum(mine, mine_too), 1, 0)
    return late + 2 * source_late + 4 * before


def diagonal_kernel(lanes, scale, sources, order, query, packed, top, total, acc, codes, known, arrived):
    copy = pltpu.make_async_copy(order, known, arrived)
    copy.start()
    blocks = [(packed[slot, 0], packed[slot, 1]) for slot in range(2)]
    queries = [rows_of(query, slot) for slot in range(2)]
    parts = [score(queries[slot], [blocks[slot]], lanes, scale, True) for slot in range(2)]
    for slot in range(2):
        store((top, total, acc), slot, weigh(parts[slot], [blocks[slot]], lanes, None))
    copy.wait()
    me = lax.axis_index("seq")
    row = lax.broadcasted_iota(jnp.int32, codes.shape, 0)
    value = jnp.zeros(codes.shape, jnp.int32)
    for place, table in enumerate(sources):
        value = jnp.where(row == place, order_of(known, me, pick(table, me)), value)
    codes[...] = value


def split(code):
    return code % 2, (code // 2) % 2, code // 4


def code_of(codes, number):
    return codes[number : number + 1, 0:1][0, 0]


def remote(lanes, scale, code, query, take, extra, refs, emit):
    late, source_late, before = split(code)
    early = 1 - late
    more = [extra(early)] if extra else []

    @pl.when(before == 1)
    def _():
        block = take(1 - source_late)
        early_parts = score(rows_of(query, early), [block], lanes, scale, False)
        late_parts = score(rows_of(query, late), [block, *more], lanes, scale, False)
        early_state = weigh(early_parts, [block], lanes, load(refs, early))
        late_state = weigh(late_parts, [block, *more], lanes, load(refs, late))
        emit(early, early_state)
        emit(late, late_state)

    @pl.when(before == 0)
    def _():
        emit(early, load(refs, early))
        blocks = [take(0), take(1), *more]
        emit(late, attend(rows_of(query, late), blocks, lanes, scale, load(refs, late), False))


def finish(result, staged, out, slot, done):
    staged[slot] = result.astype(staged.dtype)
    half = staged.shape[1]
    rows = pl.ds(pl.multiple_of(slot * half, half), half)
    pltpu.make_async_copy(staged.at[slot], out.at[rows], done.at[slot]).start()


def settle(staged, out, done):
    half = staged.shape[1]
    for slot in range(2):
        rows = pl.ds(slot * half, half)
        pltpu.make_async_copy(staged.at[slot], out.at[rows], done.at[slot]).wait()


def block_of(packed):
    return lambda slot: (packed[slot, 0], packed[slot, 1])


def stage_kernel(number, lanes, scale, codes, query, *rest):
    blocks, before, after = rest[:-6], rest[-6:-3], rest[-3:]
    extra = block_of(blocks[1]) if len(blocks) > 1 else None

    def emit(slot, state):
        store(after, slot, state)

    code = code_of(codes, number)
    remote(lanes, scale, code, query, block_of(blocks[0]), extra, before, emit)


def weights_kernel(number, lanes, scale, codes, query, keys, top, total, acc, spread, base):
    refs = (top, total, acc)
    late, source_late, before = split(code_of(codes, number))
    early = 1 - late

    @pl.when(before == 1)
    def _():
        block = (keys[1 - source_late, 0], None)
        parts = [score(rows_of(query, slot), [block], lanes, scale, False) for slot in range(2)]
        for slot in range(2):
            _, _, factor, weights = soften(parts[slot], lanes, load(refs, slot), True)
            spread[slot] = weights.T
            base[slot] = (acc[slot] * factor).T

    @pl.when(before == 0)
    def _():
        blocks = [(keys[slot, 0], None) for slot in range(2)]
        parts = score(rows_of(query, late), blocks, lanes, scale, False)
        _, _, factor, weights = soften(parts, lanes, load(refs, late), True)
        half = weights.shape[0] // 2
        spread[0] = weights[:half].T
        spread[1] = weights[half:].T
        base[late] = (acc[late] * factor).T
        base[early] = (acc[early] * (1.0 / total[early])).T


def values_kernel(number, lanes, scale, codes, near, far, spread, base, out, staged, done):
    chosen = pick(CHOICE, lax.axis_index("seq"))
    late, source_late, before = split(code_of(codes, number))

    def times(slot, source_slot):
        value = jnp.where(chosen == 0, near[source_slot, 0], far[source_slot, 0])
        return jnp.dot(spread[slot], value, preferred_element_type=jnp.float32)

    @pl.when(before == 1)
    def _():
        for slot in range(2):
            finish(base[slot] + times(slot, 1 - source_late), staged, out, slot, done)

    @pl.when(before == 0)
    def _():
        finish(base[1 - late], staged, out, 1 - late, done)
        finish(base[late] + times(0, 0) + times(1, 1), staged, out, late, done)

    settle(staged, out, done)


def gathered_kernel(lanes, scale, order, query, packed, blocks, *rest):
    before, out, staged, done, refs = rest[:3], rest[3], rest[4], rest[5], rest[6:]
    me = lax.axis_index("seq")
    count = blocks.shape[0]
    late = jnp.where(order[2 * me] < order[2 * me + 1], 1, 0)
    early = 1 - late
    store(refs, early, load(before, early))
    own = (packed[early, 0], packed[early, 1])
    store(refs, late, attend(rows_of(query, late), [own], lanes, scale, load(before, late), False))

    def emit(slot, state):
        store(refs, slot, state)

    def step(index, carry):
        source = lax.rem(me + index, count)
        take = block_of(blocks.at[source])
        remote(lanes, scale, order_of(order, me, source), query, take, None, refs, emit)
        return carry

    lax.fori_loop(1, count, step, 0)
    _, total, acc = refs
    for slot in range(2):
        finish((acc[slot] * (1.0 / total[slot])).T, staged, out, slot, done)
    settle(staged, out, done)


def on_device(queries, keys, values, block_order):
    tokens, heads, width = queries.shape
    groups = keys.shape[1]
    half = tokens // 2
    devices = lax.axis_size("seq")
    scale = width ** (-0.5) * LOG2E
    lanes = (groups, heads)
    rows = tokens * heads
    query = queries.reshape(rows, width)

    def pack(array):
        split = array.reshape(2, half, groups, width)
        return jnp.transpose(split, (0, 2, 1, 3)).reshape(2, 1, groups * half, width)

    halves = {"keys": pack(keys), "values": pack(values)}
    packed = jnp.concatenate([halves["keys"], halves["values"]], axis=1)
    shapes = [
        jax.ShapeDtypeStruct((2, 1, rows // 2), jnp.float32),
        jax.ShapeDtypeStruct((2, 1, rows // 2), jnp.float32),
        jax.ShapeDtypeStruct((2, width, rows // 2), jnp.float32),
    ]
    result = jax.ShapeDtypeStruct((rows, width), queries.dtype)
    staging = [
        pltpu.VMEM((2, rows // 2, width), queries.dtype),
        pltpu.SemaphoreType.DMA((2,)),
    ]
    vmem = pl.BlockSpec(memory_space=pltpu.VMEM)
    smem = pl.BlockSpec(memory_space=pltpu.SMEM)
    anywhere = pl.BlockSpec(memory_space=pl.ANY)

    def call(kernel, tasks, inputs, specs, out_shape, out_specs, scratch=()):
        return pl.pallas_call(
            functools.partial(kernel, lanes, scale),
            out_shape=out_shape,
            in_specs=specs + [vmem] * (len(inputs) - len(specs)),
            out_specs=out_specs,
            scratch_shapes=scratch,
            compiler_params=pltpu.CompilerParams(vmem_limit_bytes=16 * 2**20),
            cost_estimate=pl.CostEstimate(
                flops=4 * tasks * groups * half * rows // 2 * width,
                bytes_accessed=rows * width * 2,
                transcendentals=tasks * half * rows,
            ),
        )(*inputs)

    def diagonal(sources):
        def kernel(lanes, scale, *refs):
            diagonal_kernel(lanes, scale, sources, *refs)

        codes = jax.ShapeDtypeStruct((8, 128), jnp.int32)
        scratch = [pltpu.SMEM(block_order.shape, jnp.int32), pltpu.SemaphoreType.DMA]
        inputs = [block_order, query, packed]
        return call(kernel, 2, inputs, [anywhere], [*shapes, codes], [vmem] * 4, scratch)

    if devices == len(CHOICE):
        mine = tuple(range(devices))
        held = {name: mine for name in ("packed", *halves)}
        got = {"packed": packed, **halves}
        for name, sent, pairs in ROUTE:
            source = dict((target, origin) for origin, target in pairs)
            held[name] = tuple(held[sent][source[i]] for i in range(devices))
            value = got[sent]
            if name in LAST_VALUES and value.shape[1] > 1:
                value = value[:, 1:]
            got[name] = lax.ppermute(value, "seq", pairs)
        *state, codes = diagonal([held[name] for name in (*WHOLE, LAST_KEYS)])
        for stage, name in enumerate(WHOLE):
            blocks = [got[name]] if stage else [got[name], packed]
            kernel = functools.partial(stage_kernel, stage)
            inputs = [codes, query, *blocks, *state]
            state = call(kernel, 3, inputs, [], shapes, [vmem] * 3)
        kernel = functools.partial(weights_kernel, len(WHOLE))
        spread = jax.ShapeDtypeStruct((2, rows // 2, groups * half), jnp.bfloat16)
        base = jax.ShapeDtypeStruct((2, rows // 2, width), jnp.float32)
        inputs = [codes, query, got[LAST_KEYS], *state]
        state = call(kernel, 1, inputs, [], [spread, base], [vmem] * 2)
        kernel = functools.partial(values_kernel, len(WHOLE))
        inputs = [codes, *[got[name] for name in LAST_VALUES], *state]
        out = call(kernel, 1, inputs, [], result, anywhere, staging)
    else:
        blocks = lax.all_gather(packed, "seq", axis=0, tiled=False)
        *state, _ = diagonal([])
        inputs = [block_order, query, packed, blocks, *state]
        scratch = staging + [pltpu.VMEM(s.shape, s.dtype) for s in shapes]
        out = call(gathered_kernel, 2 * devices, inputs, [smem], result, anywhere, scratch)
    return out.reshape(tokens, heads, width)


def solution(mesh):
    placed = (
        P(("grp", "seq"), "head", None),
        P(("grp", "seq"), "head", None),
        P(("grp", "seq"), "head", None),
        P("grp"),
    )

    return jax.shard_map(
        on_device,
        mesh=mesh,
        in_specs=placed,
        out_specs=P(("grp", "seq"), "head", None),
        check_vma=False,
    )
```

```python
import functools

import jax
import jax.numpy as jnp
from jax import lax
from jax.experimental import pallas as pl
from jax.experimental.pallas import tpu as pltpu
from jax.sharding import PartitionSpec as P


ROUTE = (
    ("o1", "packed", ((0, 2), (3, 1), (1, 0), (2, 3))),
    ("o2", "packed", ((1, 3), (2, 0), (0, 1), (3, 2))),
    ("x", "keys", ((0, 3), (3, 0), (1, 2), (2, 1))),
    ("z", "o1", ((0, 1), (1, 0), (2, 3), (3, 2))),
    ("y", "values", ((1, 2), (2, 1), (0, 0), (3, 3))),
)
WHOLE = ("o1", "o2")
LAST_KEYS = "x"
LAST_VALUES = ("z", "y")
CHOICE = (0, 1, 1, 0)
LOW = -1e30
LOG2E = 1.4426950408889634


def pick(table, index):
    value = jnp.int32(table[0])
    for place in range(1, len(table)):
        value = jnp.where(index == place, jnp.int32(table[place]), value)
    return value


def score(query, blocks, lanes, scale, diagonal):
    groups, per_token = lanes
    rows = query.shape[0]
    keys = blocks[0][0].shape[0] // groups
    lane = lax.broadcasted_iota(jnp.int32, (keys, rows), 1)
    group = (lane % per_token) // (per_token // groups)
    parts = []
    for key, _ in blocks:
        both = lax.dot_general(
            key, query, (((1,), (1,)), ((), ())), preferred_element_type=jnp.float32
        )
        part = both[:keys]
        for g in range(1, groups):
            part = jnp.where(group == g, both[g * keys : (g + 1) * keys], part)
        part = part * scale
        if diagonal:
            place = lax.broadcasted_iota(jnp.int32, (keys, rows), 0)
            part = jnp.where(place <= lane // per_token, part, LOW)
        parts.append(part)
    return parts


def soften(parts, lanes, state, divide=False):
    groups, per_token = lanes
    lane = lax.broadcasted_iota(jnp.int32, parts[0].shape, 1)
    group = (lane % per_token) // (per_token // groups)
    top = functools.reduce(jnp.maximum, [jnp.max(part, axis=0, keepdims=True) for part in parts])
    if state is not None:
        top = jnp.maximum(top, state[0])
    parts = [jnp.exp2(part - top) for part in parts]
    total = sum(jnp.sum(weights, axis=0, keepdims=True) for weights in parts)
    factor = None
    if state is not None:
        factor = jnp.exp2(state[0] - top)
        total = state[1] * factor + total
    if divide:
        inverse = 1.0 / total
        factor = factor * inverse
        parts = [weights * inverse for weights in parts]
    spread = []
    for weights in parts:
        rounded = weights.astype(jnp.bfloat16)
        nothing = jnp.zeros_like(rounded)
        spread += [jnp.where(group == g, rounded, nothing) for g in range(groups)]
    return top, total, factor, jnp.concatenate(spread, axis=0)


def multiply(value, spread):
    return lax.dot_general(
        value, spread, (((0,), (0,)), ((), ())), preferred_element_type=jnp.float32
    )


def weigh(parts, blocks, lanes, state):
    top, total, factor, spread = soften(parts, lanes, state)
    product = multiply(jnp.concatenate([value for _, value in blocks], axis=0), spread)
    if state is None:
        return top, total, product
    return top, total, state[2] * factor + product


def attend(query, blocks, lanes, scale, state, diagonal):
    return weigh(score(query, blocks, lanes, scale, diagonal), blocks, lanes, state)


def load(refs, slot):
    return tuple(ref[slot] for ref in refs)


def store(refs, slot, state):
    for ref, part in zip(refs, state, strict=True):
        ref[slot] = part


def rows_of(ref, slot):
    half = ref.shape[0] // 2
    return ref[pl.ds(pl.multiple_of(slot * half, half), half), :]


def order_of(order, me, source):
    mine, theirs = order[2 * me], order[2 * source]
    mine_too, theirs_too = order[2 * me + 1], order[2 * source + 1]
    late = jnp.where(mine < mine_too, 1, 0)
    source_late = jnp.where(theirs < theirs_too, 1, 0)
    before = jnp.where(jnp.minimum(theirs, theirs_too) < jnp.minimum(mine, mine_too), 1, 0)
    return late + 2 * source_late + 4 * before


def diagonal_kernel(lanes, scale, sources, order, query, packed, top, total, acc, codes, known, arrived):
    copy = pltpu.make_async_copy(order, known, arrived)
    copy.start()
    blocks = [(packed[slot, 0], packed[slot, 1]) for slot in range(2)]
    queries = [rows_of(query, slot) for slot in range(2)]
    parts = [score(queries[slot], [blocks[slot]], lanes, scale, True) for slot in range(2)]
    for slot in range(2):
        store((top, total, acc), slot, weigh(parts[slot], [blocks[slot]], lanes, None))
    copy.wait()
    me = lax.axis_index("seq")
    row = lax.broadcasted_iota(jnp.int32, codes.shape, 0)
    value = jnp.zeros(codes.shape, jnp.int32)
    for place, table in enumerate(sources):
        value = jnp.where(row == place, order_of(known, me, pick(table, me)), value)
    codes[...] = value


def split(code):
    return code % 2, (code // 2) % 2, code // 4


def code_of(codes, number):
    return codes[number : number + 1, 0:1][0, 0]


def remote(lanes, scale, code, query, take, extra, refs, emit):
    late, source_late, before = split(code)
    early = 1 - late
    more = [extra(early)] if extra else []

    @pl.when(before == 1)
    def _():
        block = take(1 - source_late)
        early_parts = score(rows_of(query, early), [block], lanes, scale, False)
        late_parts = score(rows_of(query, late), [block, *more], lanes, scale, False)
        early_state = weigh(early_parts, [block], lanes, load(refs, early))
        late_state = weigh(late_parts, [block, *more], lanes, load(refs, late))
        emit(early, early_state)
        emit(late, late_state)

    @pl.when(before == 0)
    def _():
        emit(early, load(refs, early))
        blocks = [take(0), take(1), *more]
        emit(late, attend(rows_of(query, late), blocks, lanes, scale, load(refs, late), False))


def finish(result, staged, out, slot, done):
    staged[slot] = result.astype(staged.dtype)
    half = staged.shape[1]
    rows = pl.ds(pl.multiple_of(slot * half, half), half)
    pltpu.make_async_copy(staged.at[slot], out.at[rows], done.at[slot]).start()


def settle(staged, out, done):
    half = staged.shape[1]
    for slot in range(2):
        rows = pl.ds(slot * half, half)
        pltpu.make_async_copy(staged.at[slot], out.at[rows], done.at[slot]).wait()


def block_of(packed):
    return lambda slot: (packed[slot, 0], packed[slot, 1])


def stage_kernel(number, lanes, scale, codes, query, *rest):
    blocks, before, after = rest[:-6], rest[-6:-3], rest[-3:]
    extra = block_of(blocks[1]) if len(blocks) > 1 else None

    def emit(slot, state):
        store(after, slot, state)

    code = code_of(codes, number)
    remote(lanes, scale, code, query, block_of(blocks[0]), extra, before, emit)


def weights_kernel(number, lanes, scale, codes, query, keys, top, total, acc, spread, base):
    refs = (top, total, acc)
    late, source_late, before = split(code_of(codes, number))
    early = 1 - late

    @pl.when(before == 1)
    def _():
        block = (keys[1 - source_late, 0], None)
        parts = [score(rows_of(query, slot), [block], lanes, scale, False) for slot in range(2)]
        for slot in range(2):
            _, _, factor, weights = soften(parts[slot], lanes, load(refs, slot), True)
            spread[slot] = weights.T
            base[slot] = acc[slot] * factor

    @pl.when(before == 0)
    def _():
        blocks = [(keys[slot, 0], None) for slot in range(2)]
        parts = score(rows_of(query, late), blocks, lanes, scale, False)
        _, _, factor, weights = soften(parts, lanes, load(refs, late), True)
        half = weights.shape[0] // 2
        spread[0] = weights[:half].T
        spread[1] = weights[half:].T
        base[late] = acc[late] * factor
        base[early] = acc[early] * (1.0 / total[early])


def values_kernel(number, lanes, scale, codes, near, far, spread, base, out, staged, done):
    chosen = pick(CHOICE, lax.axis_index("seq"))
    late, source_late, before = split(code_of(codes, number))

    def times(slot, source_slot):
        value = jnp.where(chosen == 0, near[source_slot, 0], far[source_slot, 0])
        return jnp.dot(spread[slot], value, preferred_element_type=jnp.float32)

    @pl.when(before == 1)
    def _():
        for slot in range(2):
            finish(base[slot].T + times(slot, 1 - source_late), staged, out, slot, done)

    @pl.when(before == 0)
    def _():
        finish(base[1 - late].T, staged, out, 1 - late, done)
        finish(base[late].T + times(0, 0) + times(1, 1), staged, out, late, done)

    settle(staged, out, done)


def gathered_kernel(lanes, scale, order, query, packed, blocks, *rest):
    before, out, staged, done, refs = rest[:3], rest[3], rest[4], rest[5], rest[6:]
    me = lax.axis_index("seq")
    count = blocks.shape[0]
    late = jnp.where(order[2 * me] < order[2 * me + 1], 1, 0)
    early = 1 - late
    store(refs, early, load(before, early))
    own = (packed[early, 0], packed[early, 1])
    store(refs, late, attend(rows_of(query, late), [own], lanes, scale, load(before, late), False))

    def emit(slot, state):
        store(refs, slot, state)

    def step(index, carry):
        source = lax.rem(me + index, count)
        take = block_of(blocks.at[source])
        remote(lanes, scale, order_of(order, me, source), query, take, None, refs, emit)
        return carry

    lax.fori_loop(1, count, step, 0)
    _, total, acc = refs
    for slot in range(2):
        finish((acc[slot] * (1.0 / total[slot])).T, staged, out, slot, done)
    settle(staged, out, done)


def on_device(queries, keys, values, block_order):
    tokens, heads, width = queries.shape
    groups = keys.shape[1]
    half = tokens // 2
    devices = lax.axis_size("seq")
    scale = width ** (-0.5) * LOG2E
    lanes = (groups, heads)
    rows = tokens * heads
    query = queries.reshape(rows, width)

    def pack(array):
        split = array.reshape(2, half, groups, width)
        return jnp.transpose(split, (0, 2, 1, 3)).reshape(2, 1, groups * half, width)

    halves = {"keys": pack(keys), "values": pack(values)}
    packed = jnp.concatenate([halves["keys"], halves["values"]], axis=1)
    shapes = [
        jax.ShapeDtypeStruct((2, 1, rows // 2), jnp.float32),
        jax.ShapeDtypeStruct((2, 1, rows // 2), jnp.float32),
        jax.ShapeDtypeStruct((2, width, rows // 2), jnp.float32),
    ]
    result = jax.ShapeDtypeStruct((rows, width), queries.dtype)
    staging = [
        pltpu.VMEM((2, rows // 2, width), queries.dtype),
        pltpu.SemaphoreType.DMA((2,)),
    ]
    vmem = pl.BlockSpec(memory_space=pltpu.VMEM)
    smem = pl.BlockSpec(memory_space=pltpu.SMEM)
    anywhere = pl.BlockSpec(memory_space=pl.ANY)

    def call(kernel, tasks, inputs, specs, out_shape, out_specs, scratch=()):
        return pl.pallas_call(
            functools.partial(kernel, lanes, scale),
            out_shape=out_shape,
            in_specs=specs + [vmem] * (len(inputs) - len(specs)),
            out_specs=out_specs,
            scratch_shapes=scratch,
            compiler_params=pltpu.CompilerParams(vmem_limit_bytes=16 * 2**20),
            cost_estimate=pl.CostEstimate(
                flops=4 * tasks * groups * half * rows // 2 * width,
                bytes_accessed=rows * width * 2,
                transcendentals=tasks * half * rows,
            ),
        )(*inputs)

    def diagonal(sources):
        def kernel(lanes, scale, *refs):
            diagonal_kernel(lanes, scale, sources, *refs)

        codes = jax.ShapeDtypeStruct((8, 128), jnp.int32)
        scratch = [pltpu.SMEM(block_order.shape, jnp.int32), pltpu.SemaphoreType.DMA]
        inputs = [block_order, query, packed]
        return call(kernel, 2, inputs, [anywhere], [*shapes, codes], [vmem] * 4, scratch)

    if devices == len(CHOICE):
        mine = tuple(range(devices))
        held = {name: mine for name in ("packed", *halves)}
        got = {"packed": packed, **halves}
        for name, sent, pairs in ROUTE:
            source = dict((target, origin) for origin, target in pairs)
            held[name] = tuple(held[sent][source[i]] for i in range(devices))
            value = got[sent]
            if name in LAST_VALUES and value.shape[1] > 1:
                value = value[:, 1:]
            got[name] = lax.ppermute(value, "seq", pairs)
        *state, codes = diagonal([held[name] for name in (*WHOLE, LAST_KEYS)])
        for stage, name in enumerate(WHOLE):
            blocks = [got[name]] if stage else [got[name], packed]
            kernel = functools.partial(stage_kernel, stage)
            inputs = [codes, query, *blocks, *state]
            state = call(kernel, 3, inputs, [], shapes, [vmem] * 3)
        kernel = functools.partial(weights_kernel, len(WHOLE))
        spread = jax.ShapeDtypeStruct((2, rows // 2, groups * half), jnp.bfloat16)
        inputs = [codes, query, got[LAST_KEYS], *state]
        state = call(kernel, 1, inputs, [], [spread, shapes[2]], [vmem] * 2)
        kernel = functools.partial(values_kernel, len(WHOLE))
        inputs = [codes, *[got[name] for name in LAST_VALUES], *state]
        out = call(kernel, 1, inputs, [], result, anywhere, staging)
    else:
        blocks = lax.all_gather(packed, "seq", axis=0, tiled=False)
        *state, _ = diagonal([])
        inputs = [block_order, query, packed, blocks, *state]
        scratch = staging + [pltpu.VMEM(s.shape, s.dtype) for s in shapes]
        out = call(gathered_kernel, 2 * devices, inputs, [smem], result, anywhere, scratch)
    return out.reshape(tokens, heads, width)


def solution(mesh):
    placed = (
        P(("grp", "seq"), "head", None),
        P(("grp", "seq"), "head", None),
        P(("grp", "seq"), "head", None),
        P("grp"),
    )

    return jax.shard_map(
        on_device,
        mesh=mesh,
        in_specs=placed,
        out_specs=P(("grp", "seq"), "head", None),
        check_vma=False,
    )
```

```python
import functools

import jax
import jax.numpy as jnp
from jax import lax
from jax.experimental import pallas as pl
from jax.experimental.pallas import tpu as pltpu
from jax.sharding import PartitionSpec as P


ROUTE = (
    ("o1", "packed", ((0, 2), (3, 1), (1, 0), (2, 3))),
    ("o2", "packed", ((1, 3), (2, 0), (0, 1), (3, 2))),
    ("x", "keys", ((0, 3), (3, 0), (1, 2), (2, 1))),
    ("z", "o1", ((0, 1), (1, 0), (2, 3), (3, 2))),
    ("y", "values", ((1, 2), (2, 1), (0, 0), (3, 3))),
)
WHOLE = ("o1", "o2")
LAST_KEYS = "x"
LAST_VALUES = ("z", "y")
CHOICE = (0, 1, 1, 0)
LOW = -1e30
LOG2E = 1.4426950408889634


def pick(table, index):
    value = jnp.int32(table[0])
    for place in range(1, len(table)):
        value = jnp.where(index == place, jnp.int32(table[place]), value)
    return value


def score(query, blocks, lanes, scale, diagonal):
    groups, per_token = lanes
    rows = query.shape[0]
    keys = blocks[0][0].shape[0] // groups
    lane = lax.broadcasted_iota(jnp.int32, (keys, rows), 1)
    group = (lane % per_token) // (per_token // groups)
    parts = []
    for key, _ in blocks:
        both = lax.dot_general(
            key, query, (((1,), (1,)), ((), ())), preferred_element_type=jnp.float32
        )
        part = both[:keys]
        for g in range(1, groups):
            part = jnp.where(group == g, both[g * keys : (g + 1) * keys], part)
        part = part * scale
        if diagonal:
            place = lax.broadcasted_iota(jnp.int32, (keys, rows), 0)
            part = jnp.where(place <= lane // per_token, part, LOW)
        parts.append(part)
    return parts


def soften(parts, lanes, state):
    groups, per_token = lanes
    lane = lax.broadcasted_iota(jnp.int32, parts[0].shape, 1)
    group = (lane % per_token) // (per_token // groups)
    top = functools.reduce(jnp.maximum, [jnp.max(part, axis=0, keepdims=True) for part in parts])
    if state is not None:
        top = jnp.maximum(top, state[0])
    total = 0.0
    spread = []
    for part in parts:
        weights = jnp.exp2(part - top)
        total = total + jnp.sum(weights, axis=0, keepdims=True)
        rounded = weights.astype(jnp.bfloat16)
        nothing = jnp.zeros_like(rounded)
        spread += [jnp.where(group == g, rounded, nothing) for g in range(groups)]
    factor = None
    if state is not None:
        factor = jnp.exp2(state[0] - top)
        total = state[1] * factor + total
    return top, total, factor, jnp.concatenate(spread, axis=0)


def multiply(value, spread):
    return lax.dot_general(
        value, spread, (((0,), (0,)), ((), ())), preferred_element_type=jnp.float32
    )


def weigh(parts, blocks, lanes, state):
    top, total, factor, spread = soften(parts, lanes, state)
    product = multiply(jnp.concatenate([value for _, value in blocks], axis=0), spread)
    if state is None:
        return top, total, product
    return top, total, state[2] * factor + product


def attend(query, blocks, lanes, scale, state, diagonal):
    return weigh(score(query, blocks, lanes, scale, diagonal), blocks, lanes, state)


def load(refs, slot):
    return tuple(ref[slot] for ref in refs)


def store(refs, slot, state):
    for ref, part in zip(refs, state, strict=True):
        ref[slot] = part


def rows_of(ref, slot):
    half = ref.shape[0] // 2
    return ref[pl.ds(pl.multiple_of(slot * half, half), half), :]


def order_of(order, me, source):
    mine, theirs = order[2 * me], order[2 * source]
    mine_too, theirs_too = order[2 * me + 1], order[2 * source + 1]
    late = jnp.where(mine < mine_too, 1, 0)
    source_late = jnp.where(theirs < theirs_too, 1, 0)
    before = jnp.where(jnp.minimum(theirs, theirs_too) < jnp.minimum(mine, mine_too), 1, 0)
    return late + 2 * source_late + 4 * before


def diagonal_kernel(lanes, scale, sources, order, query, packed, top, total, acc, codes, known, arrived):
    copy = pltpu.make_async_copy(order, known, arrived)
    copy.start()
    blocks = [(packed[slot, 0], packed[slot, 1]) for slot in range(2)]
    queries = [rows_of(query, slot) for slot in range(2)]
    parts = [score(queries[slot], [blocks[slot]], lanes, scale, True) for slot in range(2)]
    for slot in range(2):
        store((top, total, acc), slot, weigh(parts[slot], [blocks[slot]], lanes, None))
    copy.wait()
    me = lax.axis_index("seq")
    row = lax.broadcasted_iota(jnp.int32, codes.shape, 0)
    value = jnp.zeros(codes.shape, jnp.int32)
    for place, table in enumerate(sources):
        value = jnp.where(row == place, order_of(known, me, pick(table, me)), value)
    codes[...] = value


def split(code):
    return code % 2, (code // 2) % 2, code // 4


def code_of(codes, number):
    return codes[number : number + 1, 0:1][0, 0]


def remote(lanes, scale, code, query, take, extra, refs, emit):
    late, source_late, before = split(code)
    early = 1 - late
    more = [extra(early)] if extra else []

    @pl.when(before == 1)
    def _():
        block = take(1 - source_late)
        early_parts = score(rows_of(query, early), [block], lanes, scale, False)
        late_parts = score(rows_of(query, late), [block, *more], lanes, scale, False)
        early_state = weigh(early_parts, [block], lanes, load(refs, early))
        late_state = weigh(late_parts, [block, *more], lanes, load(refs, late))
        emit(early, early_state)
        emit(late, late_state)

    @pl.when(before == 0)
    def _():
        emit(early, load(refs, early))
        blocks = [take(0), take(1), *more]
        emit(late, attend(rows_of(query, late), blocks, lanes, scale, load(refs, late), False))


def finish(result, staged, out, slot, done):
    staged[slot] = result.astype(staged.dtype).T
    half = staged.shape[1]
    rows = pl.ds(pl.multiple_of(slot * half, half), half)
    pltpu.make_async_copy(staged.at[slot], out.at[rows], done.at[slot]).start()


def settle(staged, out, done):
    half = staged.shape[1]
    for slot in range(2):
        rows = pl.ds(slot * half, half)
        pltpu.make_async_copy(staged.at[slot], out.at[rows], done.at[slot]).wait()


def block_of(packed):
    return lambda slot: (packed[slot, 0], packed[slot, 1])


def stage_kernel(number, lanes, scale, codes, query, *rest):
    blocks, before, after = rest[:-6], rest[-6:-3], rest[-3:]
    extra = block_of(blocks[1]) if len(blocks) > 1 else None

    def emit(slot, state):
        store(after, slot, state)

    code = code_of(codes, number)
    remote(lanes, scale, code, query, block_of(blocks[0]), extra, before, emit)


def weights_kernel(number, lanes, scale, codes, query, keys, top, total, acc, spread, share, base):
    refs = (top, total, acc)
    late, source_late, before = split(code_of(codes, number))
    early = 1 - late

    @pl.when(before == 1)
    def _():
        block = (keys[1 - source_late, 0], None)
        parts = [score(rows_of(query, slot), [block], lanes, scale, False) for slot in range(2)]
        for slot in range(2):
            _, new_total, factor, weights = soften(parts[slot], lanes, load(refs, slot))
            inverse = 1.0 / new_total
            spread[slot] = weights
            share[slot] = inverse
            base[slot] = acc[slot] * (factor * inverse)

    @pl.when(before == 0)
    def _():
        blocks = [(keys[slot, 0], None) for slot in range(2)]
        parts = score(rows_of(query, late), blocks, lanes, scale, False)
        _, new_total, factor, weights = soften(parts, lanes, load(refs, late))
        inverse = 1.0 / new_total
        half = weights.shape[0] // 2
        spread[0] = weights[:half]
        spread[1] = weights[half:]
        share[late] = inverse
        base[late] = acc[late] * (factor * inverse)
        base[early] = acc[early] * (1.0 / total[early])


def values_kernel(number, lanes, scale, codes, near, far, spread, share, base, out, staged, done):
    chosen = pick(CHOICE, lax.axis_index("seq"))
    late, source_late, before = split(code_of(codes, number))

    def take(slot):
        return jnp.where(chosen == 0, near[slot, 0], far[slot, 0])

    @pl.when(before == 1)
    def _():
        value = take(1 - source_late)
        products = [multiply(value, spread[slot]) for slot in range(2)]
        for slot in range(2):
            finish(base[slot] + products[slot] * share[slot], staged, out, slot, done)

    @pl.when(before == 0)
    def _():
        finish(base[1 - late], staged, out, 1 - late, done)
        value = jnp.concatenate([take(0), take(1)], axis=0)
        product = multiply(value, jnp.concatenate([spread[0], spread[1]], axis=0))
        finish(base[late] + product * share[late], staged, out, late, done)

    settle(staged, out, done)


def gathered_kernel(lanes, scale, order, query, packed, blocks, *rest):
    before, out, staged, done, refs = rest[:3], rest[3], rest[4], rest[5], rest[6:]
    me = lax.axis_index("seq")
    count = blocks.shape[0]
    late = jnp.where(order[2 * me] < order[2 * me + 1], 1, 0)
    early = 1 - late
    store(refs, early, load(before, early))
    own = (packed[early, 0], packed[early, 1])
    store(refs, late, attend(rows_of(query, late), [own], lanes, scale, load(before, late), False))

    def emit(slot, state):
        store(refs, slot, state)

    def step(index, carry):
        source = lax.rem(me + index, count)
        take = block_of(blocks.at[source])
        remote(lanes, scale, order_of(order, me, source), query, take, None, refs, emit)
        return carry

    lax.fori_loop(1, count, step, 0)
    _, total, acc = refs
    for slot in range(2):
        finish(acc[slot] * (1.0 / total[slot]), staged, out, slot, done)
    settle(staged, out, done)


def together_kernel(keys, values, out, done):
    copies = []
    for which, source in enumerate((keys, values)):
        copies.append(pltpu.make_async_copy(source, out.at[which], done.at[which]))
        copies[-1].start()
    for copy in copies:
        copy.wait()


def together(keys, values):
    hbm = pl.BlockSpec(memory_space=pltpu.HBM)
    return pl.pallas_call(
        together_kernel,
        out_shape=jax.ShapeDtypeStruct((2, *keys.shape), keys.dtype),
        in_specs=[hbm, hbm],
        out_specs=pl.BlockSpec(memory_space=pltpu.VMEM),
        scratch_shapes=[pltpu.SemaphoreType.DMA((2,))],
        compiler_params=pltpu.CompilerParams(vmem_limit_bytes=16 * 2**20),
    )(
        pltpu.with_memory_space_constraint(keys, pltpu.HBM),
        pltpu.with_memory_space_constraint(values, pltpu.HBM),
    )


def on_device(queries, keys, values, block_order):
    tokens, heads, width = queries.shape
    groups = keys.shape[1]
    half = tokens // 2
    devices = lax.axis_size("seq")
    scale = width ** (-0.5) * LOG2E
    lanes = (groups, heads)
    rows = tokens * heads
    query = queries.reshape(rows, width)

    raw = together(keys, values)

    def arrange(array):
        split = array.reshape(array.shape[0], 2, half, groups, width)
        turned = jnp.transpose(split, (1, 0, 3, 2, 4))
        return turned.reshape(2, array.shape[0], groups * half, width)

    packed = arrange(raw)
    shapes = [
        jax.ShapeDtypeStruct((2, 1, rows // 2), jnp.float32),
        jax.ShapeDtypeStruct((2, 1, rows // 2), jnp.float32),
        jax.ShapeDtypeStruct((2, width, rows // 2), jnp.float32),
    ]
    result = jax.ShapeDtypeStruct((rows, width), queries.dtype)
    staging = [
        pltpu.VMEM((2, rows // 2, width), queries.dtype),
        pltpu.SemaphoreType.DMA((2,)),
    ]
    vmem = pl.BlockSpec(memory_space=pltpu.VMEM)
    smem = pl.BlockSpec(memory_space=pltpu.SMEM)
    anywhere = pl.BlockSpec(memory_space=pl.ANY)

    def call(kernel, tasks, inputs, specs, out_shape, out_specs, scratch=()):
        return pl.pallas_call(
            functools.partial(kernel, lanes, scale),
            out_shape=out_shape,
            in_specs=specs + [vmem] * (len(inputs) - len(specs)),
            out_specs=out_specs,
            scratch_shapes=scratch,
            compiler_params=pltpu.CompilerParams(vmem_limit_bytes=16 * 2**20),
            cost_estimate=pl.CostEstimate(
                flops=4 * tasks * groups * half * rows // 2 * width,
                bytes_accessed=rows * width * 2,
                transcendentals=tasks * half * rows,
            ),
        )(*inputs)

    def diagonal(sources):
        def kernel(lanes, scale, *refs):
            diagonal_kernel(lanes, scale, sources, *refs)

        codes = jax.ShapeDtypeStruct((8, 128), jnp.int32)
        scratch = [pltpu.SMEM(block_order.shape, jnp.int32), pltpu.SemaphoreType.DMA]
        order = pltpu.with_memory_space_constraint(block_order, pltpu.HBM)
        inputs = [order, query, packed]
        return call(kernel, 2, inputs, [anywhere], [*shapes, codes], [vmem] * 4, scratch)

    if devices == len(CHOICE):
        mine = tuple(range(devices))
        got = {"packed": raw, "keys": raw[:1], "values": raw[1:]}
        held = {name: mine for name in got}
        for name, sent, pairs in ROUTE:
            source = dict((target, origin) for origin, target in pairs)
            held[name] = tuple(held[sent][source[i]] for i in range(devices))
            value = got[sent]
            if name in LAST_VALUES and value.shape[0] > 1:
                value = value[1:]
            got[name] = lax.ppermute(value, "seq", pairs)

        def when(name, state):
            value, state = lax.optimization_barrier((got[name], state))
            return arrange(value), state

        *state, codes = diagonal([held[name] for name in (*WHOLE, LAST_KEYS)])
        for stage, name in enumerate(WHOLE):
            block, state = when(name, state)
            blocks = [block] if stage else [block, packed]
            kernel = functools.partial(stage_kernel, stage)
            inputs = [codes, query, *blocks, *state]
            state = call(kernel, 3, inputs, [], shapes, [vmem] * 3)
        kernel = functools.partial(weights_kernel, len(WHOLE))
        spread = jax.ShapeDtypeStruct((2, groups * half, rows // 2), jnp.bfloat16)
        block, state = when(LAST_KEYS, state)
        inputs = [codes, query, block, *state]
        state = call(kernel, 1, inputs, [], [spread, *shapes[1:]], [vmem] * 3)
        kernel = functools.partial(values_kernel, len(WHOLE))
        near, state = when(LAST_VALUES[0], state)
        far, state = when(LAST_VALUES[1], state)
        inputs = [codes, near, far, *state]
        out = call(kernel, 1, inputs, [], result, anywhere, staging)
    else:
        blocks = lax.all_gather(packed, "seq", axis=0, tiled=False)
        *state, _ = diagonal([])
        inputs = [block_order, query, packed, blocks, *state]
        scratch = staging + [pltpu.VMEM(s.shape, s.dtype) for s in shapes]
        out = call(gathered_kernel, 2 * devices, inputs, [smem], result, anywhere, scratch)
    return out.reshape(tokens, heads, width)


def solution(mesh):
    placed = (
        P(("grp", "seq"), "head", None),
        P(("grp", "seq"), "head", None),
        P(("grp", "seq"), "head", None),
        P("grp"),
    )

    return jax.shard_map(
        on_device,
        mesh=mesh,
        in_specs=placed,
        out_specs=P(("grp", "seq"), "head", None),
        check_vma=False,
    )
```

```python
import functools

import jax
import jax.numpy as jnp
from jax import lax
from jax.experimental import pallas as pl
from jax.experimental.pallas import tpu as pltpu
from jax.sharding import PartitionSpec as P


ROUTE = (
    ("o1", "packed", ((0, 2), (3, 1), (1, 0), (2, 3))),
    ("o2", "packed", ((1, 3), (2, 0), (0, 1), (3, 2))),
    ("x", "keys", ((0, 3), (3, 0), (1, 2), (2, 1))),
    ("z", "o1", ((0, 1), (1, 0), (2, 3), (3, 2))),
    ("y", "values", ((1, 2), (2, 1), (0, 0), (3, 3))),
)
WHOLE = ("o1", "o2")
LAST_KEYS = "x"
LAST_VALUES = ("z", "y")
CHOICE = (0, 1, 1, 0)
LOW = -1e30
LOG2E = 1.4426950408889634


def pick(table, index):
    value = jnp.int32(table[0])
    for place in range(1, len(table)):
        value = jnp.where(index == place, jnp.int32(table[place]), value)
    return value


def score(query, blocks, lanes, scale, diagonal):
    groups, per_token = lanes
    rows = query.shape[0]
    keys = blocks[0][0].shape[0] // groups
    lane = lax.broadcasted_iota(jnp.int32, (keys, rows), 1)
    group = (lane % per_token) // (per_token // groups)
    parts = []
    for key, _ in blocks:
        both = lax.dot_general(
            key, query, (((1,), (1,)), ((), ())), preferred_element_type=jnp.float32
        )
        part = both[:keys]
        for g in range(1, groups):
            part = jnp.where(group == g, both[g * keys : (g + 1) * keys], part)
        part = part * scale
        if diagonal:
            place = lax.broadcasted_iota(jnp.int32, (keys, rows), 0)
            part = jnp.where(place <= lane // per_token, part, LOW)
        parts.append(part)
    return parts


def soften(parts, lanes, state):
    groups, per_token = lanes
    lane = lax.broadcasted_iota(jnp.int32, parts[0].shape, 1)
    group = (lane % per_token) // (per_token // groups)
    top = functools.reduce(jnp.maximum, [jnp.max(part, axis=0, keepdims=True) for part in parts])
    if state is not None:
        top = jnp.maximum(top, state[0])
    total = 0.0
    spread = []
    for part in parts:
        weights = jnp.exp2(part - top)
        total = total + jnp.sum(weights, axis=0, keepdims=True)
        rounded = weights.astype(jnp.bfloat16)
        nothing = jnp.zeros_like(rounded)
        spread += [jnp.where(group == g, rounded, nothing) for g in range(groups)]
    factor = None
    if state is not None:
        factor = jnp.exp2(state[0] - top)
        total = state[1] * factor + total
    return top, total, factor, jnp.concatenate(spread, axis=0)


def multiply(value, spread):
    return lax.dot_general(
        value, spread, (((0,), (0,)), ((), ())), preferred_element_type=jnp.float32
    )


def weigh(parts, blocks, lanes, state):
    top, total, factor, spread = soften(parts, lanes, state)
    product = multiply(jnp.concatenate([value for _, value in blocks], axis=0), spread)
    if state is None:
        return top, total, product
    return top, total, state[2] * factor + product


def attend(query, blocks, lanes, scale, state, diagonal):
    return weigh(score(query, blocks, lanes, scale, diagonal), blocks, lanes, state)


def load(refs, slot):
    return tuple(ref[slot] for ref in refs)


def store(refs, slot, state):
    for ref, part in zip(refs, state, strict=True):
        ref[slot] = part


def rows_of(ref, slot):
    half = ref.shape[0] // 2
    return ref[pl.ds(pl.multiple_of(slot * half, half), half), :]


def order_of(order, me, source):
    mine, theirs = order[2 * me], order[2 * source]
    mine_too, theirs_too = order[2 * me + 1], order[2 * source + 1]
    late = jnp.where(mine < mine_too, 1, 0)
    source_late = jnp.where(theirs < theirs_too, 1, 0)
    before = jnp.where(jnp.minimum(theirs, theirs_too) < jnp.minimum(mine, mine_too), 1, 0)
    return late + 2 * source_late + 4 * before


def diagonal_kernel(lanes, scale, sources, order, query, packed, top, total, acc, codes, known, arrived):
    copy = pltpu.make_async_copy(order, known, arrived)
    copy.start()
    blocks = [(packed[slot, 0], packed[slot, 1]) for slot in range(2)]
    queries = [rows_of(query, slot) for slot in range(2)]
    parts = [score(queries[slot], [blocks[slot]], lanes, scale, True) for slot in range(2)]
    for slot in range(2):
        store((top, total, acc), slot, weigh(parts[slot], [blocks[slot]], lanes, None))
    copy.wait()
    me = lax.axis_index("seq")
    row = lax.broadcasted_iota(jnp.int32, codes.shape, 0)
    value = jnp.zeros(codes.shape, jnp.int32)
    for place, table in enumerate(sources):
        value = jnp.where(row == place, order_of(known, me, pick(table, me)), value)
    codes[...] = value


def split(code):
    return code % 2, (code // 2) % 2, code // 4


def code_of(codes, number):
    return codes[number : number + 1, 0:1][0, 0]


def remote(lanes, scale, code, query, take, extra, refs, emit):
    late, source_late, before = split(code)
    early = 1 - late
    more = [extra(early)] if extra else []

    @pl.when(before == 1)
    def _():
        block = take(1 - source_late)
        early_parts = score(rows_of(query, early), [block], lanes, scale, False)
        late_parts = score(rows_of(query, late), [block, *more], lanes, scale, False)
        early_state = weigh(early_parts, [block], lanes, load(refs, early))
        late_state = weigh(late_parts, [block, *more], lanes, load(refs, late))
        emit(early, early_state)
        emit(late, late_state)

    @pl.when(before == 0)
    def _():
        emit(early, load(refs, early))
        blocks = [take(0), take(1), *more]
        emit(late, attend(rows_of(query, late), blocks, lanes, scale, load(refs, late), False))


def finish(result, staged, out, slot, done):
    staged[slot] = result.astype(staged.dtype).T
    half = staged.shape[1]
    rows = pl.ds(pl.multiple_of(slot * half, half), half)
    pltpu.make_async_copy(staged.at[slot], out.at[rows], done.at[slot]).start()


def settle(staged, out, done):
    half = staged.shape[1]
    for slot in range(2):
        rows = pl.ds(slot * half, half)
        pltpu.make_async_copy(staged.at[slot], out.at[rows], done.at[slot]).wait()


def block_of(packed):
    return lambda slot: (packed[slot, 0], packed[slot, 1])


def stage_kernel(number, lanes, scale, codes, query, *rest):
    blocks, before, after = rest[:-6], rest[-6:-3], rest[-3:]
    extra = block_of(blocks[1]) if len(blocks) > 1 else None

    def emit(slot, state):
        store(after, slot, state)

    code = code_of(codes, number)
    remote(lanes, scale, code, query, block_of(blocks[0]), extra, before, emit)


def weights_kernel(number, lanes, scale, codes, query, keys, top, total, acc, spread, share, base):
    refs = (top, total, acc)
    late, source_late, before = split(code_of(codes, number))
    early = 1 - late

    @pl.when(before == 1)
    def _():
        block = (keys[1 - source_late, 0], None)
        parts = [score(rows_of(query, slot), [block], lanes, scale, False) for slot in range(2)]
        for slot in range(2):
            _, new_total, factor, weights = soften(parts[slot], lanes, load(refs, slot))
            inverse = 1.0 / new_total
            spread[slot] = weights
            share[slot] = inverse
            base[slot] = acc[slot] * (factor * inverse)

    @pl.when(before == 0)
    def _():
        blocks = [(keys[slot, 0], None) for slot in range(2)]
        parts = score(rows_of(query, late), blocks, lanes, scale, False)
        _, new_total, factor, weights = soften(parts, lanes, load(refs, late))
        inverse = 1.0 / new_total
        half = weights.shape[0] // 2
        spread[0] = weights[:half]
        spread[1] = weights[half:]
        share[late] = inverse
        base[late] = acc[late] * (factor * inverse)
        base[early] = acc[early] * (1.0 / total[early])


def values_kernel(number, lanes, scale, codes, near, far, spread, share, base, out, staged, done):
    chosen = pick(CHOICE, lax.axis_index("seq"))
    late, source_late, before = split(code_of(codes, number))

    def take(slot):
        return jnp.where(chosen == 0, near[slot, 0], far[slot, 0])

    @pl.when(before == 1)
    def _():
        value = take(1 - source_late)
        products = [multiply(value, spread[slot]) for slot in range(2)]
        for slot in range(2):
            finish(base[slot] + products[slot] * share[slot], staged, out, slot, done)

    @pl.when(before == 0)
    def _():
        finish(base[1 - late], staged, out, 1 - late, done)
        value = jnp.concatenate([take(0), take(1)], axis=0)
        product = multiply(value, jnp.concatenate([spread[0], spread[1]], axis=0))
        finish(base[late] + product * share[late], staged, out, late, done)

    settle(staged, out, done)


def gathered_kernel(lanes, scale, order, query, packed, blocks, *rest):
    before, out, staged, done, refs = rest[:3], rest[3], rest[4], rest[5], rest[6:]
    me = lax.axis_index("seq")
    count = blocks.shape[0]
    late = jnp.where(order[2 * me] < order[2 * me + 1], 1, 0)
    early = 1 - late
    store(refs, early, load(before, early))
    own = (packed[early, 0], packed[early, 1])
    store(refs, late, attend(rows_of(query, late), [own], lanes, scale, load(before, late), False))

    def emit(slot, state):
        store(refs, slot, state)

    def step(index, carry):
        source = lax.rem(me + index, count)
        take = block_of(blocks.at[source])
        remote(lanes, scale, order_of(order, me, source), query, take, None, refs, emit)
        return carry

    lax.fori_loop(1, count, step, 0)
    _, total, acc = refs
    for slot in range(2):
        finish(acc[slot] * (1.0 / total[slot]), staged, out, slot, done)
    settle(staged, out, done)


def together_kernel(keys, values, out, first, second, done):
    copies = []
    pairs = ((keys, out.at[0]), (values, out.at[1]), (keys, first.at[0]), (values, second.at[0]))
    for which, (source, target) in enumerate(pairs):
        copies.append(pltpu.make_async_copy(source, target, done.at[which]))
        copies[-1].start()
    for copy in copies:
        copy.wait()


def together(keys, values):
    hbm = pl.BlockSpec(memory_space=pltpu.HBM)
    return pl.pallas_call(
        together_kernel,
        out_shape=[jax.ShapeDtypeStruct((n, *keys.shape), keys.dtype) for n in (2, 1, 1)],
        in_specs=[hbm, hbm],
        out_specs=[pl.BlockSpec(memory_space=pltpu.VMEM)] * 3,
        scratch_shapes=[pltpu.SemaphoreType.DMA((4,))],
        compiler_params=pltpu.CompilerParams(vmem_limit_bytes=16 * 2**20),
    )(
        pltpu.with_memory_space_constraint(keys, pltpu.HBM),
        pltpu.with_memory_space_constraint(values, pltpu.HBM),
    )


def on_device(queries, keys, values, block_order):
    tokens, heads, width = queries.shape
    groups = keys.shape[1]
    half = tokens // 2
    devices = lax.axis_size("seq")
    scale = width ** (-0.5) * LOG2E
    lanes = (groups, heads)
    rows = tokens * heads
    query = queries.reshape(rows, width)

    raw, raw_keys, raw_values = together(keys, values)

    def arrange(array):
        split = array.reshape(array.shape[0], 2, half, groups, width)
        turned = jnp.transpose(split, (1, 0, 3, 2, 4))
        return turned.reshape(2, array.shape[0], groups * half, width)

    packed = arrange(raw)
    shapes = [
        jax.ShapeDtypeStruct((2, 1, rows // 2), jnp.float32),
        jax.ShapeDtypeStruct((2, 1, rows // 2), jnp.float32),
        jax.ShapeDtypeStruct((2, width, rows // 2), jnp.float32),
    ]
    result = jax.ShapeDtypeStruct((rows, width), queries.dtype)
    staging = [
        pltpu.VMEM((2, rows // 2, width), queries.dtype),
        pltpu.SemaphoreType.DMA((2,)),
    ]
    vmem = pl.BlockSpec(memory_space=pltpu.VMEM)
    smem = pl.BlockSpec(memory_space=pltpu.SMEM)
    anywhere = pl.BlockSpec(memory_space=pl.ANY)

    def call(kernel, tasks, inputs, specs, out_shape, out_specs, scratch=()):
        return pl.pallas_call(
            functools.partial(kernel, lanes, scale),
            out_shape=out_shape,
            in_specs=specs + [vmem] * (len(inputs) - len(specs)),
            out_specs=out_specs,
            scratch_shapes=scratch,
            compiler_params=pltpu.CompilerParams(vmem_limit_bytes=16 * 2**20),
            cost_estimate=pl.CostEstimate(
                flops=4 * tasks * groups * half * rows // 2 * width,
                bytes_accessed=rows * width * 2,
                transcendentals=tasks * half * rows,
            ),
        )(*inputs)

    def diagonal(sources):
        def kernel(lanes, scale, *refs):
            diagonal_kernel(lanes, scale, sources, *refs)

        codes = jax.ShapeDtypeStruct((8, 128), jnp.int32)
        scratch = [pltpu.SMEM(block_order.shape, jnp.int32), pltpu.SemaphoreType.DMA]
        order = pltpu.with_memory_space_constraint(block_order, pltpu.HBM)
        inputs = [order, query, packed]
        return call(kernel, 2, inputs, [anywhere], [*shapes, codes], [vmem] * 4, scratch)

    if devices == len(CHOICE):
        mine = tuple(range(devices))
        got = {"packed": raw, "keys": raw_keys, "values": raw_values}
        held = {name: mine for name in got}
        for name, sent, pairs in ROUTE:
            source = dict((target, origin) for origin, target in pairs)
            held[name] = tuple(held[sent][source[i]] for i in range(devices))
            value = got[sent]
            if name in LAST_VALUES and value.shape[0] > 1:
                value = value[1:]
            got[name] = lax.ppermute(value, "seq", pairs)

        def when(name, state):
            value, state = lax.optimization_barrier((got[name], state))
            return arrange(value), state

        *state, codes = diagonal([held[name] for name in (*WHOLE, LAST_KEYS)])
        for stage, name in enumerate(WHOLE):
            block, state = when(name, state)
            blocks = [block] if stage else [block, packed]
            kernel = functools.partial(stage_kernel, stage)
            inputs = [codes, query, *blocks, *state]
            state = call(kernel, 3, inputs, [], shapes, [vmem] * 3)
        kernel = functools.partial(weights_kernel, len(WHOLE))
        spread = jax.ShapeDtypeStruct((2, groups * half, rows // 2), jnp.bfloat16)
        block, state = when(LAST_KEYS, state)
        inputs = [codes, query, block, *state]
        state = call(kernel, 1, inputs, [], [spread, *shapes[1:]], [vmem] * 3)
        kernel = functools.partial(values_kernel, len(WHOLE))
        near, state = when(LAST_VALUES[0], state)
        far, state = when(LAST_VALUES[1], state)
        inputs = [codes, near, far, *state]
        out = call(kernel, 1, inputs, [], result, anywhere, staging)
    else:
        blocks = lax.all_gather(packed, "seq", axis=0, tiled=False)
        *state, _ = diagonal([])
        inputs = [block_order, query, packed, blocks, *state]
        scratch = staging + [pltpu.VMEM(s.shape, s.dtype) for s in shapes]
        out = call(gathered_kernel, 2 * devices, inputs, [smem], result, anywhere, scratch)
    return out.reshape(tokens, heads, width)


def solution(mesh):
    placed = (
        P(("grp", "seq"), "head", None),
        P(("grp", "seq"), "head", None),
        P(("grp", "seq"), "head", None),
        P("grp"),
    )

    return jax.shard_map(
        on_device,
        mesh=mesh,
        in_specs=placed,
        out_specs=P(("grp", "seq"), "head", None),
        check_vma=False,
    )
```
